256 devices in a mesh: gx: 8 (over z_lo, core), gy: 4 (over y), gz: 8 (over z_hi, x).
Axes of the slice: x: 4, y: 4, z: 8 (z_hi: 2, z_lo: 4; z = z_hi * 4 + z_lo), core: 2. Of those that a mesh axis runs over, the one named last changes fastest.
Arguments:
- raw_weight: float32 [128, 27, 128], P(('gx', 'gy')), may hold values from -6 to 6
- inputs: bfloat16 [64, 64, 128, 128], P('gx', 'gy', 'gz'), may hold values from -6 to 6
- cotangent: bfloat16 [64, 64, 128, 128], P('gx', 'gy', 'gz'), may hold values from -0.099609375 to 0.099609375
Outputs:
- input_grad: bfloat16 [64, 64, 128, 128], P('gx', 'gy', 'gz')
- weight_grad: float32 [128, 27, 128], P(('gx', 'gy'))
The draws below stay inside these ranges and needn't reach their ends.
All inputs are finite; a program needn't handle non-finite values.
Results may differ from the reference program's by a relative error of at most 0.0049.
Values may be sent and summed in bfloat16 or wider, within the bound.
A program may use at most 64 MiB of HBM per device.

```python
import math
import jax
import jax.numpy as jnp
from jax import lax

C = 128
KK = 27
NX = 64
NY = 64
NZ = 128


def draw_raw_weight(key, part):
    sub_keys = jax.random.split(key, 4)
    row_scale = jnp.exp(jax.random.uniform(sub_keys[0], (C, 1, 1), jnp.float32, math.log(0.1), 0.0))
    col_scale = jnp.exp(jax.random.uniform(sub_keys[1], (1, 1, C), jnp.float32, math.log(0.1), 0.0))
    col_mean = jax.random.uniform(sub_keys[2], (1, 1, C), jnp.float32, -0.5, 0.5)
    base_draw = jnp.clip(jax.random.normal(sub_keys[3], (C, KK, C), jnp.float32), -4.0, 4.0)
    return jnp.clip((base_draw * row_scale + col_mean) * col_scale, -6.0, 6.0)


def steps_of(rng, shape, cuts, smallest, top_value):
    def one(dim, parts):
        steps = jax.random.uniform(jax.random.fold_in(jax.random.fold_in(rng, 6), dim), (parts,), jnp.float32, smallest / len(cuts), top_value / len(cuts))
        return jnp.repeat(jnp.exp(steps), shape[dim] // parts).reshape((-1,) + (1,) * (len(shape) - dim - 1))

    level = one(*cuts[0])
    for cut in cuts[1:]:
        level = level * one(*cut)
    return level


def normal_values(rng, shape, scale, most, shards=(), dtype=jnp.bfloat16):
    array = jax.random.normal(rng, shape, jnp.float32) * scale
    if len(shards) > 0:
        array = steps_of(rng, shape, shards, -0.22, 0.18) * array
    return jnp.clip(array, min=-most, max=most).astype(dtype)


def setup_inputs(seed: int = 0) -> dict:
    key_of = jax.random.split(jax.random.key(seed), 4)
    raw_weight = draw_raw_weight(jax.random.fold_in(key_of[3], 71), 0)
    inputs = normal_values(key_of[1], (NX, NY, NZ, C), 1.0, 6.0, ((0, 8), (1, 4), (2, 8)))
    cotangent = normal_values(key_of[2], (NX, NY, NZ, C), 0.017, 0.099609375, ((0, 8), (1, 4), (2, 8)))
    return dict(raw_weight=raw_weight, inputs=inputs, cotangent=cotangent)


var_eps = 1e-05
norm_eps = 1e-06
clip_norm = 600.0

def tap_view(padded, tap_a, tap_b, tap_c, extent):
    view = padded[2 - tap_a:2 - tap_a + extent[0], 2 - tap_b:2 - tap_b + extent[1], 2 - tap_c:2 - tap_c + extent[2], :]
    return view.reshape(-1, view.shape[-1])

def reference(raw_weight, inputs, cotangent):
    extent = inputs.shape[:3]
    channels = inputs.shape[3]
    fan_count = raw_weight.shape[0] * raw_weight.shape[1]
    sum_first = lax.optimization_barrier(jnp.sum(raw_weight, axis=(0, 1)))
    sum_second = lax.optimization_barrier(jnp.sum(raw_weight * raw_weight, axis=(0, 1)))
    mean_out = sum_first / fan_count
    var_out = sum_second / fan_count - mean_out * mean_out
    inv_std = lax.rsqrt(var_out + var_eps)
    std_float = (raw_weight - mean_out) * inv_std
    std_half = lax.optimization_barrier(std_float.astype(jnp.bfloat16)).astype(jnp.float32)
    padded = jnp.pad(cotangent.astype(jnp.float32), ((1, 1), (1, 1), (1, 1), (0, 0)))
    flat_in = inputs.astype(jnp.float32).reshape(-1, channels)
    dx_total = jnp.zeros((flat_in.shape[0], channels), jnp.float32)
    pieces = []
    for tap_a in range(3):
        for tap_b in range(3):
            for tap_c in range(3):
                tap_index = tap_a * 9 + tap_b * 3 + tap_c
                view = tap_view(padded, tap_a, tap_b, tap_c, extent)
                dx_total = dx_total + jnp.dot(view, std_half[:, tap_index, :].T, precision=lax.Precision.HIGHEST)
                pieces.append(jnp.dot(flat_in.T, view, precision=lax.Precision.HIGHEST))
    input_grad = dx_total.reshape(extent[0], extent[1], extent[2], channels).astype(jnp.bfloat16)
    filter_grad = jnp.stack(pieces, axis=1)
    mean_grad = lax.optimization_barrier(jnp.sum(filter_grad, axis=(0, 1))) / fan_count
    mean_cross = lax.optimization_barrier(jnp.sum(filter_grad * std_float, axis=(0, 1))) / fan_count
    raw_grad = inv_std * (filter_grad - mean_grad - std_float * mean_cross)
    square_sum = jnp.sum(raw_grad * raw_grad)
    scale = jnp.minimum(1.0, clip_norm * lax.rsqrt(square_sum + norm_eps))
    return (input_grad, raw_grad * scale)
```

```python
import functools

import jax
import jax.numpy as jnp
from jax import lax
from jax.experimental import pallas as pl
from jax.experimental.pallas import tpu as pltpu
from jax.sharding import PartitionSpec as P

var_eps = 1e-05
norm_eps = 1e-06
clip_norm = 600.0
F32 = jnp.float32
BF16 = jnp.bfloat16
MESH = pl.DeviceIdType.MESH
AXES = ("gx", "gy", "gz")

NCORE, NZL, NYC, NXC, NZH = 2, 4, 4, 4, 2
NZR = NZL * NZH
CHUNKS = ((0, 8, 2, 0), (8, 8, 2, 2), (16, 11, 3, 4))
SLOTS = 7


def kernel(raw_hbm, in_hbm, cot_hbm, dx_hbm, wg_ref, *scratch):
    (raw_ref, in_ref, shifted, face_out, edge_out, face_in, edge_in, corner_in, in_t, part, recv_c, send_xy, recv_xy,
     recv_z, full, std, wz, w_all, w_cat, dx_ref, stats_w, stats_g,
     load_sem, halo_send, halo_recv, c_send, c_recv, xy_send, xy_recv, z_send, z_recv, x_send, x_recv,
     w1_send, w1_recv, w2_send, w2_recv, w3_send, w3_recv, sw_send, sw_recv, sg_send, sg_recv) = scratch
    taps, rows, chan = raw_ref.shape
    ex, ey, ez = in_ref.shape[:3]
    fan_count = float(rows * NCORE * NZL * NYC * taps)
    count = {"gx": NCORE * NZL, "gy": NYC, "gz": NXC * NZH}
    me = {axis: lax.axis_index(axis) for axis in AXES}
    core, zl = lax.rem(me["gx"], NCORE), lax.div(me["gx"], NCORE)
    my = me["gy"]
    mx, zh = lax.rem(me["gz"], NXC), lax.div(me["gz"], NXC)
    mz = zh * NZL + zl

    def spot(c=None, x=None, y=None, z=None):
        c = core if c is None else c
        x = mx if x is None else x
        y = my if y is None else y
        z = mz if z is None else z
        return {"gx": lax.rem(z, NZL) * NCORE + c, "gy": y, "gz": lax.div(z, NZL) * NXC + x}

    partner = spot(c=1 - core)

    def plane_peer(k):
        flat = lax.rem(me["gx"] * NYC + my + k, 32)
        return {"gx": lax.div(flat, NYC), "gy": lax.rem(flat, NYC)}

    def xy_peer(k):
        flat = lax.rem(my * NXC + mx + k, NXC * NYC)
        return lax.rem(flat, NXC), lax.div(flat, NXC)

    flat_g = (my * NXC + mx) * NCORE + core

    def stat_peer(k):
        flat = lax.rem(flat_g + k, 32)
        where = lax.div(flat, NCORE)
        return spot(c=lax.rem(flat, NCORE), x=lax.rem(where, NXC), y=lax.div(where, NXC))

    def z_peer(k):
        return spot(z=lax.rem(mz + k, NZR))

    def remote(src, dst, send_sem, recv_sem, where):
        return pltpu.make_async_remote_copy(
            src_ref=src, dst_ref=dst, send_sem=send_sem, recv_sem=recv_sem,
            device_id=where, device_id_type=MESH,
        )

    sends = []

    def launch(copy):
        copy.start()
        sends.append(copy)
        return copy

    body = pl.ds(1, ey)
    load_cot = pltpu.make_async_copy(cot_hbm, shifted.at[1, pl.ds(1, ex), body], load_sem.at[0])
    load_raw = pltpu.make_async_copy(raw_hbm, raw_ref, load_sem.at[1])
    load_in = pltpu.make_async_copy(in_hbm, in_ref, load_sem.at[2])
    load_cot.start()
    load_raw.start()
    load_in.start()

    offsets = [(a, b, c) for c in (1, -1, 0) for a in (0, 1, -1) for b in (0, 1, -1) if (a, b, c) != (0, 0, 0)]

    def neighbour(off):
        return {axis: lax.rem(me[axis] + count[axis] + o, count[axis]) for axis, o in zip(AXES, off)}

    barrier = pltpu.get_barrier_semaphore()
    greeted = 0
    for off in offsets:
        if off[2] != 0:
            pl.semaphore_signal(barrier, inc=1, device_id=neighbour(off), device_id_type=MESH)
            greeted += 1
    for k in range(1, 32):
        pl.semaphore_signal(barrier, inc=1, device_id=plane_peer(k), device_id_type=MESH)
        pl.semaphore_signal(barrier, inc=1, device_id=stat_peer(k), device_id_type=MESH)
        greeted += 2
    for k in range(1, NZR):
        pl.semaphore_signal(barrier, inc=1, device_id=z_peer(k), device_id_type=MESH)
        greeted += 1

    low = {axis: me[axis] == 0 for axis in AXES}
    high = {axis: me[axis] == count[axis] - 1 for axis in AXES}
    tile = jnp.zeros((16, chan), BF16)
    for end, at_end in enumerate((low, high)):

        @pl.when(at_end["gx"])
        def _():
            shifted[1, (ex + 1) * end] = jnp.zeros((ey + 2, ez, chan), BF16)
            for side in range(2):
                face_in[side, (ex + 1) * end] = tile
                for b in range(2):
                    corner_in[side, b, end] = tile

        @pl.when(at_end["gy"])
        def _():
            shifted[1, :, (ey + 1) * end] = jnp.zeros((ex + 2, ez, chan), BF16)
            for side in range(2):
                edge_in[side, end] = tile
                for a in range(2):
                    corner_in[side, end, a] = tile

        @pl.when(at_end["gz"])
        def _():
            face_in[end] = jnp.zeros((ex + 2, ey, chan), BF16)
            edge_in[end] = jnp.zeros((2, 16, chan), BF16)
            corner_in[end] = jnp.zeros((2, 2, 16, chan), BF16)

    w_all[taps] = jnp.zeros((8, 16, chan), BF16)
    for y in range(NYC):
        send_xy[y, taps] = tile

    load_cot.wait()
    edge_rows = [[[], []], [[], []]]
    for x in range(ex):
        plane = shifted[1, x + 1, 1:ey + 1].astype(F32)
        for f, z in enumerate((0, ez - 1)):
            face = plane[:, z, :]
            face_out[f, x] = face.astype(BF16)
            edge_rows[f][0].append(face[0:1])
            edge_rows[f][1].append(face[ey - 1:ey])
    for f in range(2):
        for b in range(2):
            edge_out[f, b] = jnp.concatenate(edge_rows[f][b] + [jnp.zeros((16 - ex, chan), F32)], axis=0).astype(BF16)

    load_raw.wait()

    def per_output(value):
        return jnp.sum(jnp.sum(value, axis=0), axis=0, keepdims=True)

    raw = raw_ref[...]
    flat_w = me["gx"] * NYC + my
    stats_w[flat_w] = jnp.concatenate([per_output(raw), per_output(raw * raw), jnp.zeros((6, chan), F32)], axis=0)
    pl.semaphore_wait(barrier, greeted)

    def exists(off):
        ok = None
        for axis, o in zip(AXES, off):
            if o != 0:
                one = jnp.logical_not(high[axis] if o > 0 else low[axis])
                ok = one if ok is None else jnp.logical_and(ok, one)
        return ok

    def halo_copy(n, off):
        a, b, c = off
        near = {1: (ex, ey), -1: (1, 1)}
        if c == 0:
            xs = pl.ds(1, ex) if a == 0 else near[a][0]
            ys = body if b == 0 else near[b][1]
            xd = pl.ds(1, ex) if a == 0 else (0 if a > 0 else ex + 1)
            yd = body if b == 0 else (0 if b > 0 else ey + 1)
            src, dst = shifted.at[1, xs, ys], shifted.at[1, xd, yd]
        else:
            f, side = (1, 0) if c > 0 else (0, 1)
            if b == 0:
                xs = pl.ds(0, ex) if a == 0 else (ex - 1 if a > 0 else 0)
                xd = pl.ds(1, ex) if a == 0 else (0 if a > 0 else ex + 1)
                src, dst = face_out.at[f, xs], face_in.at[side, xd]
            else:
                src = edge_out.at[f, 1 if b > 0 else 0]
                ys = 0 if b > 0 else 1
                dst = edge_in.at[side, ys] if a == 0 else corner_in.at[side, ys, 0 if a > 0 else 1]
        return remote(src, dst, halo_send.at[n], halo_recv.at[n], neighbour(off))

    halos = [(off, halo_copy(n, off)) for n, off in enumerate(offsets)]
    for off, copy in halos:

        @pl.when(exists(off))
        def _():
            copy.start()

    def halo_wait(keep):
        for off, copy in halos:
            if keep(off):

                @pl.when(exists(tuple(-o for o in off)))
                def _():
                    copy.wait_recv()

    weight_sums = [
        launch(remote(stats_w.at[flat_w], stats_w.at[flat_w], sw_send.at[k - 1], sw_recv.at[k - 1], plane_peer(k)))
        for k in range(1, 32)
    ]

    row_i = lax.broadcasted_iota(jnp.int32, (chan, chan), 0)
    col_i = lax.broadcasted_iota(jnp.int32, (chan, chan), 1)

    def natural(i):
        return (i // 4 % 4) * 32 + (i // 64) * 16 + (i // 16 % 4) * 4 + i % 4

    to_mine = jnp.where(col_i == natural(row_i), 1.0, 0.0).astype(BF16)
    to_natural = jnp.where(row_i == natural(col_i), 1.0, 0.0).astype(BF16)

    load_in.wait()
    for x in range(ex):
        block = in_ref[x].reshape(ey * ez, chan)
        in_t[:, x * ey * ez:(x + 1) * ey * ez] = lax.dot_general(
            to_mine, block, (((1,), (1,)), ((), ())), preferred_element_type=F32
        ).astype(BF16)

    order = [t for c in (1, 0, 2) for t in range(c, taps, 3)]

    def view(t, start, planes):
        a, b, c = t // 9, (t // 3) % 3, t % 3
        block = shifted[2 - c, pl.ds(start + 2 - a, planes), 2 - b:2 - b + ey]
        return block.reshape(planes * ey * ez, chan)

    half_rows = chan // NCORE

    def filter_chunk(n):
        first, done, _, _ = CHUNKS[n]
        for u in range(first, first + done, 2):
            group = list(range(u, min(u + 2, first + done)))
            views = [view(order[v], 0, ex) for v in group]
            right = jnp.concatenate(views, axis=1) if len(views) > 1 else views[0]
            product = jnp.dot(in_t[...], right, preferred_element_type=F32)
            for j, v in enumerate(group):
                for c in range(NCORE):
                    part[c, v] = product[c * half_rows:(c + 1) * half_rows, j * chan:(j + 1) * chan]
        span = pl.ds(first, done)
        return launch(remote(part.at[1 - core, span], recv_c.at[span], c_send.at[n], c_recv.at[n], partner))

    def xy_chunk(n, copy):
        first, done, each, slot = CHUNKS[n]
        copy.wait_recv()
        for v in range(first, first + done):
            total = part[core, v] + recv_c[v]
            for y in range(NYC):
                send_xy[y, v] = total[y * 16:(y + 1) * 16].astype(BF16)
        copies = []
        for k in range(1, NXC * NYC):
            px, py = xy_peer(k)
            index = n * 15 + k - 1
            copies.append(launch(remote(
                send_xy.at[py, pl.ds(first + px * each, each)], recv_xy.at[k - 1, pl.ds(slot, each)],
                xy_send.at[index], xy_recv.at[index], spot(x=px, y=py),
            )))
        return copies

    def z_chunk(n, copies):
        first, done, each, slot = CHUNKS[n]
        for copy in copies:
            copy.wait_recv()
        span = pl.ds(slot, each)
        total = send_xy[my, pl.ds(first + mx * each, each)].astype(F32)
        for k in range(1, NXC * NYC):
            total = total + recv_xy[k - 1, span].astype(F32)
        recv_z[mz, span] = total.astype(BF16)
        return [
            launch(remote(recv_z.at[mz, span], recv_z.at[mz, span],
                          z_send.at[n * 7 + k - 1], z_recv.at[n * 7 + k - 1], z_peer(k)))
            for k in range(1, NZR)
        ]

    def shift(slot, side, amount, edge):
        depth = lax.broadcasted_iota(jnp.int32, (ey, ez, chan), 1)
        for x in range(ex + 2):
            plane = shifted[1, x, 1:ey + 1].astype(F32)
            outer = face_in[side, x].astype(F32)[:, None, :]
            shifted[slot, x, 1:ey + 1] = jnp.where(depth == edge, outer, pltpu.roll(plane, amount, 1)).astype(BF16)
        depth = lax.broadcasted_iota(jnp.int32, (ex + 2, ez, chan), 1)
        for b in range(2):
            y = (ey + 1) * b
            plane = shifted[1, :, y].astype(F32)
            outer = jnp.concatenate([
                corner_in[side, b, 0].astype(F32)[ex - 1:ex], edge_in[side, b].astype(F32)[0:ex],
                corner_in[side, b, 1].astype(F32)[0:1],
            ], axis=0)[:, None, :]
            shifted[slot, :, y] = jnp.where(depth == edge, outer, pltpu.roll(plane, amount, 1)).astype(BF16)

    halo_wait(lambda off: off[2] == 0)
    core_0 = filter_chunk(0)

    for copy in weight_sums:
        copy.wait_recv()
    sums = stats_w[0]
    for k in range(1, 32):
        sums = sums + stats_w[k]
    mean_out = sums[0:1] / fan_count
    var_out = sums[1:2] / fan_count - mean_out * mean_out
    inv_std = lax.rsqrt(var_out + var_eps)
    for u, t in enumerate(order):
        value = (raw_ref[t] - mean_out) * inv_std
        std[u] = value
        wz[zl, u] = value.astype(BF16)
    gather_z = [
        launch(remote(wz.at[zl], wz.at[zl], w1_send.at[k - 1], w1_recv.at[k - 1], spot(z=zh * NZL + lax.rem(zl + k, NZL))))
        for k in range(1, NZL)
    ]

    xy_0 = xy_chunk(0, core_0)
    halo_wait(lambda off: off[2] == -1)
    shift(2, 1, ez - 1, ez - 1)
    core_1 = filter_chunk(1)
    halo_wait(lambda off: off[2] == 1)
    shift(0, 0, 1, 0)
    xy_1 = xy_chunk(1, core_1)
    core_2 = filter_chunk(2)

    for copy in gather_z:
        copy.wait_recv()
    slab = core * NYC + my
    for u in range(taps):
        w_all[u, slab] = wz[:, u].astype(F32).reshape(16, chan).astype(BF16)
    xy_2 = xy_chunk(2, core_2)
    gather_y = [
        launch(remote(w_all.at[pl.ds(0, taps), slab], w_all.at[pl.ds(0, taps), slab],
                      w2_send.at[k - 1], w2_recv.at[k - 1], spot(y=lax.rem(my + k, NYC))))
        for k in range(1, NYC)
    ]
    z_0 = z_chunk(0, xy_0)
    z_1 = z_chunk(1, xy_1)
    z_2 = z_chunk(2, xy_2)
    for copy in gather_y:
        copy.wait_recv()
    slabs = w_all.at[pl.ds(0, taps), pl.ds(core * NYC, NYC)]
    gather_c = launch(remote(slabs, slabs, w3_send.at[0], w3_recv.at[0], partner))

    gather_c.wait_recv()
    for u in range(0, taps, 2):
        group = range(u, min(u + 2, taps))
        right = [w_all[v].reshape(chan, chan) for v in group]
        right = jnp.concatenate(right, axis=1) if len(right) > 1 else right[0]
        w_cat[:, u * chan:(u + len(group)) * chan] = jnp.dot(
            to_natural, right, preferred_element_type=F32
        ).astype(BF16)
    step = 2
    half = ex // 2

    def dx_step(n, carry):
        start = n * step
        left = jnp.concatenate([view(t, start, step) for t in order], axis=1)
        product = lax.dot_general(left, w_cat[...], (((1,), (1,)), ((), ())), preferred_element_type=F32)
        dx_ref[pl.ds(start, step)] = product.astype(BF16).reshape(step, ey, ez, chan)
        return carry

    stores = [
        pltpu.make_async_copy(dx_ref.at[pl.ds(h * half, half)], dx_hbm.at[pl.ds(h * half, half)], load_sem.at[3 + h])
        for h in range(2)
    ]
    lax.fori_loop(0, half // step, dx_step, 0)
    stores[0].start()

    for copy in z_0 + z_1 + z_2:
        copy.wait_recv()
    grad = recv_z[0].astype(F32)
    for k in range(1, NZR):
        grad = grad + recv_z[k].astype(F32)
    near = []
    for first, _, each, _ in CHUNKS:
        near += [w_all[first + mx * each + j, slab].astype(F32) for j in range(each)]
    cross = grad[0] * near[0]
    for j in range(1, SLOTS):
        cross = cross + grad[j] * near[j]
    stats_g[flat_g] = jnp.concatenate(
        [per_output(grad), jnp.sum(cross, axis=0, keepdims=True), per_output(grad * grad), jnp.zeros((5, chan), F32)],
        axis=0,
    )
    grad_sums = [
        launch(remote(stats_g.at[flat_g], stats_g.at[flat_g], sg_send.at[k - 1], sg_recv.at[k - 1], stat_peer(k)))
        for k in range(1, 32)
    ]
    for j in range(SLOTS):
        mine = grad[j, 0:rows]
        for q in range(1, NZL):
            mine = jnp.where(zl == q, grad[j, q * rows:(q + 1) * rows], mine)
        full[mx, j] = mine
    gather_x = [
        launch(remote(full.at[mx], full.at[mx], x_send.at[k - 1], x_recv.at[k - 1], spot(x=lax.rem(mx + k, NXC))))
        for k in range(1, NXC)
    ]

    lax.fori_loop(half // step, ex // step, dx_step, 0)
    stores[1].start()

    for copy in gather_x + grad_sums:
        copy.wait_recv()
    sums = stats_g[0]
    for k in range(1, 32):
        sums = sums + stats_g[k]
    sum_grad, sum_cross, sum_square = sums[0:1], sums[1:2], sums[2:3]
    mean_grad = sum_grad / fan_count
    mean_cross = sum_cross / fan_count
    spread = sum_square - 2.0 * mean_grad * sum_grad - 2.0 * mean_cross * sum_cross
    spread = (
        spread
        + fan_count * mean_grad * mean_grad
        + fan_count * mean_cross * mean_cross * var_out / (var_out + var_eps)
    )
    square_sum = jnp.sum(inv_std * inv_std * spread, axis=1, keepdims=True)
    scale = jnp.minimum(1.0, clip_norm * lax.rsqrt(square_sum + norm_eps))
    factor = inv_std * scale
    for first, done, each, slot in CHUNKS:
        for v in range(done):
            u = first + v
            wg_ref[order[u]] = factor * (full[v // each, slot + v % each] - mean_grad - std[u] * mean_cross)

    for copy in sends:
        copy.wait_send()
    for off, copy in halos:

        @pl.when(exists(off))
        def _():
            copy.wait_send()
    for copy in stores:
        copy.wait()


def on_device(raw_weight, inputs, cotangent):
    rows, taps, chan = raw_weight.shape
    ex, ey, ez = inputs.shape[:3]
    dma = pltpu.SemaphoreType.DMA

    def pair(n):
        return [dma((n,)), dma((n,))]

    scratch = [
        pltpu.VMEM((taps, rows, chan), F32),
        pltpu.VMEM(inputs.shape, BF16),
        pltpu.VMEM((3, ex + 2, ey + 2, ez, chan), BF16),
        pltpu.VMEM((2, ex, ey, chan), BF16),
        pltpu.VMEM((2, 2, 16, chan), BF16),
        pltpu.VMEM((2, ex + 2, ey, chan), BF16),
        pltpu.VMEM((2, 2, 16, chan), BF16),
        pltpu.VMEM((2, 2, 2, 16, chan), BF16),
        pltpu.VMEM((chan, ex * ey * ez), BF16),
        pltpu.VMEM((NCORE, taps, chan // NCORE, chan), F32),
        pltpu.VMEM((taps, chan // NCORE, chan), F32),
        pltpu.VMEM((NYC, taps + 1, 16, chan), BF16),
        pltpu.VMEM((NXC * NYC - 1, SLOTS, 16, chan), BF16),
        pltpu.VMEM((NZR, SLOTS, 16, chan), BF16),
        pltpu.VMEM((NXC, SLOTS, rows, chan), F32),
        pltpu.VMEM((taps, rows, chan), F32),
        pltpu.VMEM((NZL, taps, rows, chan), BF16),
        pltpu.VMEM((taps + 1, 8, 16, chan), BF16),
        pltpu.VMEM((chan, taps * chan), BF16),
        pltpu.VMEM(inputs.shape, BF16),
        pltpu.VMEM((32, 8, chan), F32),
        pltpu.VMEM((32, 8, chan), F32),
        dma((5,)), *pair(26), *pair(3), *pair(45), *pair(21), *pair(3),
        *pair(3), *pair(3), *pair(1), *pair(31), *pair(31),
    ]
    vmem = pl.BlockSpec(memory_space=pltpu.VMEM)
    anywhere = pl.BlockSpec(memory_space=pl.ANY)
    input_grad, weight_grad = pl.pallas_call(
        kernel,
        out_shape=(
            jax.ShapeDtypeStruct(cotangent.shape, BF16),
            jax.ShapeDtypeStruct((taps, rows, chan), F32),
        ),
        in_specs=[anywhere] * 3,
        out_specs=(anywhere, vmem),
        scratch_shapes=scratch,
        compiler_params=pltpu.CompilerParams(
            collective_id=0, has_side_effects=True, vmem_limit_bytes=60 * 1024 * 1024
        ),
    )(jnp.transpose(raw_weight, (1, 0, 2)), inputs, cotangent)
    return input_grad, jnp.transpose(weight_grad, (1, 0, 2))


def solution(mesh):
    in_specs = (P(("gx", "gy"), None, None), P("gx", "gy", "gz", None), P("gx", "gy", "gz", None))
    out_specs = (P("gx", "gy", "gz", None), P(("gx", "gy"), None, None))
    return jax.shard_map(
        on_device, mesh=mesh, in_specs=in_specs, out_specs=out_specs, check_vma=False
    )
```

```python
import functools

import jax
import jax.numpy as jnp
from jax import lax
from jax.experimental import pallas as pl
from jax.experimental.pallas import tpu as pltpu
from jax.sharding import PartitionSpec as P

var_eps = 1e-05
norm_eps = 1e-06
clip_norm = 600.0
F32 = jnp.float32
BF16 = jnp.bfloat16
MESH = pl.DeviceIdType.MESH
AXES = ("gx", "gy", "gz")

NCORE, NZL, NYC, NXC, NZH = 2, 4, 4, 4, 2
NZR = NZL * NZH
CHUNKS = ((0, 8, 2, 0), (8, 8, 2, 2), (16, 11, 3, 4))
SLOTS = 7


def kernel(raw_hbm, in_hbm, cot_hbm, dx_ref, wg_ref, *scratch):
    (raw_ref, in_ref, shifted, face_out, edge_out, face_in, edge_in, corner_in, in_t, part, recv_c, send_xy, recv_xy,
     recv_z, full, std, wz, w_all, w_cat, stats_w, stats_g, load_sem, halo_send, halo_recv, sems) = scratch
    taps, rows, chan = raw_ref.shape
    ex, ey, ez = in_ref.shape[:3]
    fan_count = float(rows * NCORE * NZL * NYC * taps)
    count = {"gx": NCORE * NZL, "gy": NYC, "gz": NXC * NZH}
    me = {axis: lax.axis_index(axis) for axis in AXES}
    core, zl = lax.rem(me["gx"], NCORE), lax.div(me["gx"], NCORE)
    my = me["gy"]
    mx, zh = lax.rem(me["gz"], NXC), lax.div(me["gz"], NXC)
    mz = zh * NZL + zl

    def spot(c=None, x=None, y=None, z=None):
        c = core if c is None else c
        x = mx if x is None else x
        y = my if y is None else y
        z = mz if z is None else z
        return {"gx": lax.rem(z, NZL) * NCORE + c, "gy": y, "gz": lax.div(z, NZL) * NXC + x}

    partner = spot(c=1 - core)

    def plane_peer(k):
        flat = lax.rem(me["gx"] * NYC + my + k, 32)
        return {"gx": lax.div(flat, NYC), "gy": lax.rem(flat, NYC)}

    def xy_peer(k):
        flat = lax.rem(my * NXC + mx + k, NXC * NYC)
        return lax.rem(flat, NXC), lax.div(flat, NXC)

    flat_g = (my * NXC + mx) * NCORE + core

    def stat_peer(k):
        flat = lax.rem(flat_g + k, 32)
        where = lax.div(flat, NCORE)
        return spot(c=lax.rem(flat, NCORE), x=lax.rem(where, NXC), y=lax.div(where, NXC))

    def z_peer(k):
        return spot(z=lax.rem(mz + k, NZR))

    def remote(src, dst, send_sem, recv_sem, where):
        return pltpu.make_async_remote_copy(
            src_ref=src, dst_ref=dst, send_sem=send_sem, recv_sem=recv_sem,
            device_id=where, device_id_type=MESH,
        )

    pending = []

    def group(copies, whole, send_sem, recv_sem):
        for src, dst, where in copies:
            remote(src, dst, send_sem, recv_sem, where).start()
        total = remote(whole, whole, send_sem, recv_sem, partner)
        pending.append(total)
        return total

    body = pl.ds(1, ey)
    load_cot = pltpu.make_async_copy(cot_hbm, shifted.at[1, pl.ds(1, ex), body], load_sem.at[0])
    load_raw = pltpu.make_async_copy(raw_hbm, raw_ref, load_sem.at[1])
    load_in = pltpu.make_async_copy(in_hbm, in_ref, load_sem.at[2])
    load_cot.start()
    load_raw.start()
    load_in.start()

    offsets = [(a, b, c) for c in (1, -1, 0) for a in (0, 1, -1) for b in (0, 1, -1) if (a, b, c) != (0, 0, 0)]

    def neighbour(off):
        return {axis: lax.rem(me[axis] + count[axis] + o, count[axis]) for axis, o in zip(AXES, off)}

    barrier = pltpu.get_barrier_semaphore()
    greeted = 0
    for off in offsets:
        if off[2] != 0:
            pl.semaphore_signal(barrier, inc=1, device_id=neighbour(off), device_id_type=MESH)
            greeted += 1
    for k in range(1, 32):
        pl.semaphore_signal(barrier, inc=1, device_id=plane_peer(k), device_id_type=MESH)
        greeted += 1
    for dx in range(1, NXC):
        for dy in range(NYC):
            for c in range(NCORE):
                where = spot(c=c, x=lax.rem(mx + dx, NXC), y=lax.rem(my + dy, NYC))
                pl.semaphore_signal(barrier, inc=1, device_id=where, device_id_type=MESH)
                greeted += 1
    for k in range(NZL):
        where = spot(z=(1 - zh) * NZL + lax.rem(zl + k, NZL))
        pl.semaphore_signal(barrier, inc=1, device_id=where, device_id_type=MESH)
        greeted += 1

    low = {axis: me[axis] == 0 for axis in AXES}
    high = {axis: me[axis] == count[axis] - 1 for axis in AXES}
    tile = jnp.zeros((16, chan), BF16)
    for end, at_end in enumerate((low, high)):

        @pl.when(at_end["gx"])
        def _():
            shifted[1, (ex + 1) * end] = jnp.zeros((ey + 2, ez, chan), BF16)
            for side in range(2):
                face_in[side, (ex + 1) * end] = tile
                for b in range(2):
                    corner_in[side, b, end] = tile

        @pl.when(at_end["gy"])
        def _():
            shifted[1, :, (ey + 1) * end] = jnp.zeros((ex + 2, ez, chan), BF16)
            for side in range(2):
                edge_in[side, end] = tile
                for a in range(2):
                    corner_in[side, end, a] = tile

        @pl.when(at_end["gz"])
        def _():
            face_in[end] = jnp.zeros((ex + 2, ey, chan), BF16)
            edge_in[end] = jnp.zeros((2, 16, chan), BF16)
            corner_in[end] = jnp.zeros((2, 2, 16, chan), BF16)

    w_all[taps] = jnp.zeros((8, 16, chan), BF16)
    for y in range(NYC):
        send_xy[y, taps] = tile

    with jax.named_scope('w_cot'):
        load_cot.wait()
    edge_rows = [[[], []], [[], []]]
    for x in range(ex):
        plane = shifted[1, x + 1, 1:ey + 1].astype(F32)
        for f, z in enumerate((0, ez - 1)):
            face = plane[:, z, :]
            face_out[f, x] = face.astype(BF16)
            edge_rows[f][0].append(face[0:1])
            edge_rows[f][1].append(face[ey - 1:ey])
    for f in range(2):
        for b in range(2):
            edge_out[f, b] = jnp.concatenate(edge_rows[f][b] + [jnp.zeros((16 - ex, chan), F32)], axis=0).astype(BF16)

    load_raw.wait()

    def per_output(value):
        return jnp.sum(jnp.sum(value, axis=0), axis=0, keepdims=True)

    raw = raw_ref[...]
    flat_w = me["gx"] * NYC + my
    stats_w[flat_w] = jnp.concatenate([per_output(raw), per_output(raw * raw)], axis=0)
    with jax.named_scope("w_barrier"):
        pl.semaphore_wait(barrier, greeted)

    def exists(off):
        ok = None
        for axis, o in zip(AXES, off):
            if o != 0:
                one = jnp.logical_not(high[axis] if o > 0 else low[axis])
                ok = one if ok is None else jnp.logical_and(ok, one)
        return ok

    def halo_copy(n, off):
        a, b, c = off
        near = {1: (ex, ey), -1: (1, 1)}
        if c == 0:
            xs = pl.ds(1, ex) if a == 0 else near[a][0]
            ys = body if b == 0 else near[b][1]
            xd = pl.ds(1, ex) if a == 0 else (0 if a > 0 else ex + 1)
            yd = body if b == 0 else (0 if b > 0 else ey + 1)
            src, dst = shifted.at[1, xs, ys], shifted.at[1, xd, yd]
        else:
            f, side = (1, 0) if c > 0 else (0, 1)
            if b == 0:
                xs = pl.ds(0, ex) if a == 0 else (ex - 1 if a > 0 else 0)
                xd = pl.ds(1, ex) if a == 0 else (0 if a > 0 else ex + 1)
                src, dst = face_out.at[f, xs], face_in.at[side, xd]
            else:
                src = edge_out.at[f, 1 if b > 0 else 0]
                ys = 0 if b > 0 else 1
                dst = edge_in.at[side, ys] if a == 0 else corner_in.at[side, ys, 0 if a > 0 else 1]
        return remote(src, dst, halo_send.at[n], halo_recv.at[n], neighbour(off))

    halos = [(off, halo_copy(n, off)) for n, off in enumerate(offsets)]
    for off, copy in halos:

        @pl.when(exists(off))
        def _():
            copy.start()

    def halo_wait(keep):
        for off, copy in halos:
            if keep(off):

                @pl.when(exists(tuple(-o for o in off)))
                def _():
                    copy.wait_recv()

    weight_sums = group(
        [(stats_w.at[flat_w], stats_w.at[flat_w], plane_peer(k)) for k in range(1, 32)],
        stats_w.at[pl.ds(0, 31)], sems.at[0], sems.at[1],
    )

    row_i = lax.broadcasted_iota(jnp.int32, (chan, chan), 0)
    col_i = lax.broadcasted_iota(jnp.int32, (chan, chan), 1)

    def natural(i):
        return (i // 4 % 4) * 32 + (i // 64) * 16 + (i // 16 % 4) * 4 + i % 4

    to_mine = jnp.where(col_i == natural(row_i), 1.0, 0.0).astype(BF16)
    to_natural = jnp.where(row_i == natural(col_i), 1.0, 0.0).astype(BF16)

    load_in.wait()
    for x in range(ex):
        block = in_ref[x].reshape(ey * ez, chan)
        in_t[:, x * ey * ez:(x + 1) * ey * ez] = lax.dot_general(
            to_mine, block, (((1,), (1,)), ((), ())), preferred_element_type=F32
        ).astype(BF16)

    order = [t for c in (1, 0, 2) for t in range(c, taps, 3)]

    def view(t, start, planes):
        a, b, c = t // 9, (t // 3) % 3, t % 3
        block = shifted[2 - c, pl.ds(start + 2 - a, planes), 2 - b:2 - b + ey]
        return block.reshape(planes * ey * ez, chan)

    half_rows = chan // NCORE

    def filter_chunk(n):
        first, done, _, _ = CHUNKS[n]
        for u in range(first, first + done, 2):
            both = list(range(u, min(u + 2, first + done)))
            views = [view(order[v], 0, ex) for v in both]
            right = jnp.concatenate(views, axis=1) if len(views) > 1 else views[0]
            product = jnp.dot(in_t[...], right, preferred_element_type=F32)
            for j, v in enumerate(both):
                for c in range(NCORE):
                    part[c, v] = product[c * half_rows:(c + 1) * half_rows, j * chan:(j + 1) * chan]
        span = pl.ds(first, done)
        return group(
            [(part.at[1 - core, span], recv_c.at[span], partner)], recv_c.at[span], sems.at[2 + n], sems.at[5 + n]
        )

    def xy_chunk(n, copy):
        first, done, each, slot = CHUNKS[n]
        with jax.named_scope("w_core%d" % n):
            copy.wait_recv()
        for v in range(first, first + done):
            total = part[core, v] + recv_c[v]
            for y in range(NYC):
                send_xy[y, v] = total[y * 16:(y + 1) * 16].astype(BF16)
        copies = []
        for k in range(1, NXC * NYC):
            px, py = xy_peer(k)
            copies.append((
                send_xy.at[py, pl.ds(first + px * each, each)], recv_xy.at[k - 1, pl.ds(slot, each)],
                spot(x=px, y=py),
            ))
        return group(copies, recv_xy.at[:, pl.ds(slot, each)], sems.at[8 + n], sems.at[11 + n])

    def z_chunk(n, copy):
        first, done, each, slot = CHUNKS[n]
        with jax.named_scope("w_xy%d" % n):
            copy.wait_recv()
        span = pl.ds(slot, each)
        total = send_xy[my, pl.ds(first + mx * each, each)].astype(F32)
        for k in range(1, NXC * NYC):
            total = total + recv_xy[k - 1, span].astype(F32)
        recv_z[mz, span] = total.astype(BF16)
        return group(
            [(recv_z.at[mz, span], recv_z.at[mz, span], z_peer(k)) for k in range(1, NZR)],
            recv_z.at[pl.ds(0, NZR - 1), span], sems.at[14 + n], sems.at[17 + n],
        )

    def shift(slot, side, amount, edge):
        depth = lax.broadcasted_iota(jnp.int32, (ey, ez, chan), 1)
        for x in range(ex + 2):
            plane = shifted[1, x, 1:ey + 1].astype(F32)
            outer = face_in[side, x].astype(F32)[:, None, :]
            shifted[slot, x, 1:ey + 1] = jnp.where(depth == edge, outer, pltpu.roll(plane, amount, 1)).astype(BF16)
        depth = lax.broadcasted_iota(jnp.int32, (ex + 2, ez, chan), 1)
        for b in range(2):
            y = (ey + 1) * b
            plane = shifted[1, :, y].astype(F32)
            outer = jnp.concatenate([
                corner_in[side, b, 0].astype(F32)[ex - 1:ex], edge_in[side, b].astype(F32)[0:ex],
                corner_in[side, b, 1].astype(F32)[0:1],
            ], axis=0)[:, None, :]
            shifted[slot, :, y] = jnp.where(depth == edge, outer, pltpu.roll(plane, amount, 1)).astype(BF16)

    with jax.named_scope("w_halo_xy"):
        halo_wait(lambda off: off[2] == 0)
    core_0 = filter_chunk(0)
    with jax.named_scope("w_halo_z1"):
        halo_wait(lambda off: off[2] == -1)
    shift(2, 1, ez - 1, ez - 1)
    core_1 = filter_chunk(1)
    xy_0 = xy_chunk(0, core_0)
    with jax.named_scope("w_halo_z2"):
        halo_wait(lambda off: off[2] == 1)
    shift(0, 0, 1, 0)
    core_2 = filter_chunk(2)
    xy_1 = xy_chunk(1, core_1)
    xy_2 = xy_chunk(2, core_2)

    with jax.named_scope("w_weight_sums"):
        weight_sums.wait_recv()
    sums = stats_w[0]
    for k in range(1, 32):
        sums = sums + stats_w[k]
    mean_out = sums[0:1] / fan_count
    var_out = sums[1:2] / fan_count - mean_out * mean_out
    inv_std = lax.rsqrt(var_out + var_eps)
    for u, t in enumerate(order):
        value = (raw_ref[t] - mean_out) * inv_std
        std[u] = value
        wz[zl, u] = value.astype(BF16)
    gather_z = group(
        [(wz.at[zl], wz.at[zl], spot(z=zh * NZL + lax.rem(zl + k, NZL))) for k in range(1, NZL)],
        wz.at[pl.ds(0, NZL - 1)], sems.at[20], sems.at[21],
    )

    z_0 = z_chunk(0, xy_0)
    with jax.named_scope("w_gather_z"):
        gather_z.wait_recv()
    slab = core * NYC + my
    for u in range(taps):
        w_all[u, slab] = wz[:, u].astype(F32).reshape(16, chan).astype(BF16)
    tap_span = pl.ds(0, taps)
    gather_y = group(
        [(w_all.at[tap_span, slab], w_all.at[tap_span, slab], spot(y=lax.rem(my + k, NYC))) for k in range(1, NYC)],
        w_all.at[tap_span, pl.ds(0, NYC - 1)], sems.at[22], sems.at[23],
    )
    z_1 = z_chunk(1, xy_1)
    z_2 = z_chunk(2, xy_2)
    with jax.named_scope("w_gather_y"):
        gather_y.wait_recv()
    slabs = w_all.at[tap_span, pl.ds(core * NYC, NYC)]
    gather_c = group([(slabs, slabs, partner)], slabs, sems.at[24], sems.at[25])

    with jax.named_scope("w_z"):
        z_0.wait_recv()
        z_1.wait_recv()
        z_2.wait_recv()
    grad = recv_z[0].astype(F32)
    for k in range(1, NZR):
        grad = grad + recv_z[k].astype(F32)
    near = []
    for first, _, each, _ in CHUNKS:
        near += [w_all[first + mx * each + j, slab].astype(F32) for j in range(each)]
    cross = grad[0] * near[0]
    for j in range(1, SLOTS):
        cross = cross + grad[j] * near[j]
    stats_g[flat_g] = jnp.concatenate(
        [per_output(grad), jnp.sum(cross, axis=0, keepdims=True), per_output(grad * grad), jnp.zeros((1, chan), F32)],
        axis=0,
    )
    grad_sums = group(
        [(stats_g.at[flat_g], stats_g.at[flat_g], stat_peer(k)) for k in range(1, 32)],
        stats_g.at[pl.ds(0, 31)], sems.at[26], sems.at[27],
    )
    for j in range(SLOTS):
        mine = grad[j, 0:rows]
        for q in range(1, NZL):
            mine = jnp.where(zl == q, grad[j, q * rows:(q + 1) * rows], mine)
        full[mx, j] = mine
    gather_x = group(
        [(full.at[mx], full.at[mx], spot(x=lax.rem(mx + k, NXC))) for k in range(1, NXC)],
        full.at[pl.ds(0, NXC - 1)], sems.at[28], sems.at[29],
    )

    with jax.named_scope("w_gather_c"):
        gather_c.wait_recv()
    for u in range(0, taps, 2):
        pair = range(u, min(u + 2, taps))
        right = [w_all[v].reshape(chan, chan) for v in pair]
        right = jnp.concatenate(right, axis=1) if len(right) > 1 else right[0]
        w_cat[:, u * chan:(u + len(pair)) * chan] = jnp.dot(
            to_natural, right, preferred_element_type=F32
        ).astype(BF16)
    step = 2

    def dx_step(n, carry):
        start = n * step
        left = jnp.concatenate([view(t, start, step) for t in order], axis=1)
        product = lax.dot_general(left, w_cat[...], (((1,), (1,)), ((), ())), preferred_element_type=F32)
        dx_ref[pl.ds(start, step)] = product.astype(BF16).reshape(step, ey, ez, chan)
        return carry

    with jax.named_scope("dx"):
        lax.fori_loop(0, ex // step, dx_step, 0)

    with jax.named_scope("w_grad_sums"):
        grad_sums.wait_recv()
    with jax.named_scope("w_gather_x"):
        gather_x.wait_recv()
    sums = stats_g[0]
    for k in range(1, 32):
        sums = sums + stats_g[k]
    sum_grad, sum_cross, sum_square = sums[0:1], sums[1:2], sums[2:3]
    mean_grad = sum_grad / fan_count
    mean_cross = sum_cross / fan_count
    spread = sum_square - 2.0 * mean_grad * sum_grad - 2.0 * mean_cross * sum_cross
    spread = (
        spread
        + fan_count * mean_grad * mean_grad
        + fan_count * mean_cross * mean_cross * var_out / (var_out + var_eps)
    )
    square_sum = jnp.sum(inv_std * inv_std * spread, axis=1, keepdims=True)
    scale = jnp.minimum(1.0, clip_norm * lax.rsqrt(square_sum + norm_eps))
    factor = inv_std * scale
    for first, done, each, slot in CHUNKS:
        for v in range(done):
            u = first + v
            wg_ref[order[u]] = factor * (full[v // each, slot + v % each] - mean_grad - std[u] * mean_cross)

    with jax.named_scope("w_sends"):
        for copy in pending:
            copy.wait_send()
    for off, copy in halos:

        @pl.when(exists(off))
        def _():
            copy.wait_send()


def write_out(dx_ref, wg_ref, dx_hbm, wg_hbm, sem):
    copies = [pltpu.make_async_copy(dx_ref, dx_hbm, sem.at[0]), pltpu.make_async_copy(wg_ref, wg_hbm, sem.at[1])]
    for copy in copies:
        copy.start()
    for copy in copies:
        copy.wait()


def on_device(raw_weight, inputs, cotangent):
    rows, taps, chan = raw_weight.shape
    ex, ey, ez = inputs.shape[:3]
    dma = pltpu.SemaphoreType.DMA

    scratch = [
        pltpu.VMEM((taps, rows, chan), F32),
        pltpu.VMEM(inputs.shape, BF16),
        pltpu.VMEM((3, ex + 2, ey + 2, ez, chan), BF16),
        pltpu.VMEM((2, ex, ey, chan), BF16),
        pltpu.VMEM((2, 2, 16, chan), BF16),
        pltpu.VMEM((2, ex + 2, ey, chan), BF16),
        pltpu.VMEM((2, 2, 16, chan), BF16),
        pltpu.VMEM((2, 2, 2, 16, chan), BF16),
        pltpu.VMEM((chan, ex * ey * ez), BF16),
        pltpu.VMEM((NCORE, taps, chan // NCORE, chan), F32),
        pltpu.VMEM((taps, chan // NCORE, chan), F32),
        pltpu.VMEM((NYC, taps + 1, 16, chan), BF16),
        pltpu.VMEM((NXC * NYC - 1, SLOTS, 16, chan), BF16),
        pltpu.VMEM((NZR, SLOTS, 16, chan), BF16),
        pltpu.VMEM((NXC, SLOTS, rows, chan), F32),
        pltpu.VMEM((taps, rows, chan), F32),
        pltpu.VMEM((NZL, taps, rows, chan), BF16),
        pltpu.VMEM((taps + 1, 8, 16, chan), BF16),
        pltpu.VMEM((chan, taps * chan), BF16),
        pltpu.VMEM((32, 2, chan), F32),
        pltpu.VMEM((32, 4, chan), F32),
        dma((3,)), dma((26,)), dma((26,)), dma((30,)),
    ]
    vmem = pl.BlockSpec(memory_space=pltpu.VMEM)
    anywhere = pl.BlockSpec(memory_space=pl.ANY)
    shapes = (
        jax.ShapeDtypeStruct(cotangent.shape, BF16),
        jax.ShapeDtypeStruct((taps, rows, chan), F32),
    )
    results = pl.pallas_call(
        kernel,
        out_shape=tuple(pltpu.VMEM(one.shape, one.dtype) for one in shapes),
        in_specs=[anywhere] * 3,
        out_specs=(vmem, vmem),
        scratch_shapes=scratch,
        compiler_params=pltpu.CompilerParams(
            collective_id=0, has_side_effects=True, vmem_limit_bytes=32 * 1024 * 1024
        ),
    )(*(
        pltpu.with_memory_space_constraint(one, pltpu.HBM)
        for one in (jnp.transpose(raw_weight, (1, 0, 2)), inputs, cotangent)
    ))
    input_grad, weight_grad = pl.pallas_call(
        write_out,
        out_shape=shapes,
        in_specs=[vmem, vmem],
        out_specs=(anywhere, anywhere),
        scratch_shapes=[dma((2,))],
    )(*(pltpu.with_memory_space_constraint(one, pltpu.VMEM) for one in results))
    return input_grad, jnp.transpose(weight_grad, (1, 0, 2))


def solution(mesh):
    in_specs = (P(("gx", "gy"), None, None), P("gx", "gy", "gz", None), P("gx", "gy", "gz", None))
    out_specs = (P("gx", "gy", "gz", None), P(("gx", "gy"), None, None))
    return jax.shard_map(
        on_device, mesh=mesh, in_specs=in_specs, out_specs=out_specs, check_vma=False
    )
```

```python
import functools

import jax
import jax.numpy as jnp
from jax import lax
from jax.experimental import pallas as pl
from jax.experimental.pallas import tpu as pltpu
from jax.sharding import PartitionSpec as P

var_eps = 1e-05
norm_eps = 1e-06
clip_norm = 600.0
F32 = jnp.float32
BF16 = jnp.bfloat16
MESH = pl.DeviceIdType.MESH
AXES = ("gx", "gy", "gz")

NCORE, NZL, NYC, NXC, NZH = 2, 4, 4, 4, 2
NZR = NZL * NZH
CHUNKS = ((0, 8, 2, 0), (8, 8, 2, 2), (16, 11, 3, 4))
SLOTS = 7


def kernel(raw_hbm, in_hbm, cot_hbm, dx_ref, wg_ref, *scratch):
    (raw_ref, in_ref, shifted, face_out, edge_out, corner_out, face_in, edge_in, corner_in, up_out, up_in, in_t,
     part, recv_c, send_xy, recv_xy, recv_z, full, wz, w_all, w_cat, stats_w, stats_g,
     load_sem, sends, halo_recv, recvs, hello) = scratch
    taps, rows, chan = raw_ref.shape
    ex, ey, ez = in_ref.shape[:3]
    fan_count = float(rows * NCORE * NZL * NYC * taps)
    count = {"gx": NCORE * NZL, "gy": NYC, "gz": NXC * NZH}
    me = {axis: lax.axis_index(axis) for axis in AXES}
    core, zl = lax.rem(me["gx"], NCORE), lax.div(me["gx"], NCORE)
    my = me["gy"]
    mx, zh = lax.rem(me["gz"], NXC), lax.div(me["gz"], NXC)
    mz = zh * NZL + zl

    def spot(c=None, x=None, y=None, z=None):
        c = core if c is None else c
        x = mx if x is None else x
        y = my if y is None else y
        z = mz if z is None else z
        return {"gx": lax.rem(z, NZL) * NCORE + c, "gy": y, "gz": lax.div(z, NZL) * NXC + x}

    partner = spot(c=1 - core)
    x_line = [lax.rem(mx + k, NXC) for k in range(1, NXC)]
    y_line = [lax.rem(my + k, NYC) for k in range(1, NYC)]

    def xy_peer(k):
        flat = lax.rem(my * NXC + mx + k, NXC * NYC)
        return lax.rem(flat, NXC), lax.div(flat, NXC)

    flat_g = (my * NXC + mx) * NCORE + core

    def stat_peer(k):
        flat = lax.rem(flat_g + k, 32)
        where = lax.div(flat, NCORE)
        return spot(c=lax.rem(flat, NCORE), x=lax.rem(where, NXC), y=lax.div(where, NXC))

    def z_peer(k):
        return spot(z=lax.rem(mz + k, NZR))

    def remote(src, dst, send_sem, recv_sem, where):
        return pltpu.make_async_remote_copy(
            src_ref=src, dst_ref=dst, send_sem=send_sem, recv_sem=recv_sem,
            device_id=where, device_id_type=MESH,
        )

    def group(copies, wholes, send_sem, recv_sem):
        for src, dst, where in copies:
            remote(src, dst, send_sem, recv_sem, where).start()
        return remote(wholes, wholes, send_sem, recv_sem, partner)

    body = pl.ds(1, ey)
    load_cot = pltpu.make_async_copy(cot_hbm, shifted.at[1, pl.ds(1, ex), body], load_sem.at[0])
    load_in = pltpu.make_async_copy(in_hbm, in_ref, load_sem.at[1])
    load_raw = pltpu.make_async_copy(raw_hbm, raw_ref, load_sem.at[2])
    load_cot.start()
    load_in.start()
    load_raw.start()

    low = {axis: me[axis] == 0 for axis in AXES}
    high = {axis: me[axis] == count[axis] - 1 for axis in AXES}
    plane_offs = [(a, b, 0) for a in (1, -1, 0) for b in (0, 1, -1) if (a, b) != (0, 0)]
    down_offs = [(a, b, -1) for a in (0, 1, -1) for b in (0, 1, -1)]
    up_offs = [(-a, -b, 1) for a, b, _ in down_offs]

    def neighbour(off):
        return {axis: lax.rem(me[axis] + count[axis] + o, count[axis]) for axis, o in zip(AXES, off)}

    def exists(off):
        ok = None
        for axis, o in zip(AXES, off):
            if o != 0:
                one = me[axis] < count[axis] - 1 if o > 0 else me[axis] > 0
                ok = one if ok is None else jnp.logical_and(ok, one)
        return ok

    barrier = pltpu.get_barrier_semaphore()
    for off in up_offs + plane_offs:

        @pl.when(exists(off))
        def _():
            pl.semaphore_signal(barrier, inc=1, device_id=neighbour(off), device_id_type=MESH)

    near_z = [spot(z=lax.rem(mz + k, NZR)) for k in (1, 2, NZR - 2, NZR - 1)]
    lines = [spot(c=c, x=x) for x in x_line for c in range(NCORE)]
    lines += [spot(c=c, y=y) for y in y_line for c in range(NCORE)]
    for where in near_z + lines:
        pl.semaphore_signal(barrier, inc=1, device_id=where, device_id_type=MESH)

    def sides(axis):
        return (me[axis] > 0).astype(jnp.int32), (me[axis] < count[axis] - 1).astype(jnp.int32)

    around = (1 + sum(sides("gx"))) * (1 + sum(sides("gy")))
    greeted = around - 1 + around * sides("gz")[0] + len(near_z) + len(lines)

    tile = jnp.zeros((16, chan), BF16)
    for end, at_end in enumerate((low, high)):

        @pl.when(at_end["gx"])
        def _():
            shifted[1, (ex + 1) * end] = jnp.zeros((ey + 2, ez, chan), BF16)
            for side in range(2):
                face_in[side, (ex + 1) * end] = tile
                for b in range(2):
                    corner_in[side, b, end] = jnp.zeros((2, chan), BF16)

        @pl.when(at_end["gy"])
        def _():
            shifted[1, :, (ey + 1) * end] = jnp.zeros((ex + 2, ez, chan), BF16)
            for side in range(2):
                edge_in[side, end] = jnp.zeros((ex, chan), BF16)
                for a in range(2):
                    corner_in[side, end, a] = jnp.zeros((2, chan), BF16)

        @pl.when(at_end["gz"])
        def _():
            face_in[end] = jnp.zeros((ex + 2, ey, chan), BF16)
            edge_in[end] = jnp.zeros((2, ex, chan), BF16)
            corner_in[end] = jnp.zeros((2, 2, 2, chan), BF16)
            if end:
                up_in[...] = jnp.zeros((ex, ey, chan), BF16)

    w_all[taps] = jnp.zeros((8, 16, chan), BF16)
    for y in range(NYC):
        send_xy[y, taps] = tile
    with jax.named_scope("w_cot"):
        load_cot.wait()

    def make_faces(f, z):
        firsts, lasts = [], []
        for x in range(ex):
            face = shifted[1, x + 1, 1:ey + 1].astype(F32)[:, z, :]
            face_out[f, x] = face.astype(BF16)
            firsts.append(face[0:1])
            lasts.append(face[ey - 1:ey])
        for b, edge in enumerate((firsts, lasts)):
            edge_out[f, b] = jnp.concatenate(edge, axis=0).astype(BF16)
            for a, x in enumerate((0, ex - 1)):
                corner_out[f, b, a] = jnp.concatenate([edge[x], edge[x]], axis=0).astype(BF16)

    make_faces(0, 0)
    load_in.wait()
    for x in range(ex):
        up_out[x] = in_ref[x].astype(F32)[:, 0, :].astype(BF16)
    with jax.named_scope("w_barrier"):
        pl.semaphore_wait(barrier, greeted)

    def halo_copy(n, off, send=None):
        a, b, c = off
        near = {1: (ex, ey), -1: (1, 1)}
        if c == 0:
            xs = pl.ds(1, ex) if a == 0 else near[a][0]
            ys = body if b == 0 else near[b][1]
            xd = pl.ds(1, ex) if a == 0 else (0 if a > 0 else ex + 1)
            yd = body if b == 0 else (0 if b > 0 else ey + 1)
            src, dst = shifted.at[1, xs, ys], shifted.at[1, xd, yd]
        else:
            f, side = (1, 0) if c > 0 else (0, 1)
            if b == 0:
                xs = pl.ds(0, ex) if a == 0 else (ex - 1 if a > 0 else 0)
                xd = pl.ds(1, ex) if a == 0 else (0 if a > 0 else ex + 1)
                src, dst = face_out.at[f, xs], face_in.at[side, xd]
            else:
                end, ys = (1, 0) if b > 0 else (0, 1)
                src = edge_out.at[f, end] if a == 0 else corner_out.at[f, end, 1 if a > 0 else 0]
                dst = edge_in.at[side, ys] if a == 0 else corner_in.at[side, ys, 0 if a > 0 else 1]
        return remote(src, dst, sends.at[n if send is None else send], halo_recv.at[n], neighbour(off))

    down = [(off, halo_copy(n, off)) for n, off in enumerate(down_offs)]
    down_in = [((0, 0, -1), remote(up_out, up_in, sends.at[17], halo_recv.at[17], neighbour((0, 0, -1))))]
    plane = [(off, halo_copy(9 + n, off)) for n, off in enumerate(plane_offs)]
    up = [(off, halo_copy(18 + n, off, n)) for n, off in enumerate(up_offs)]

    def halo_do(halos, act, flip):
        for off, copy in halos:

            @pl.when(exists(tuple(-o for o in off) if flip else off))
            def _():
                act(copy)

    def halo_start(halos):
        halo_do(halos, lambda copy: copy.start(), False)

    def halo_sent(halos):
        halo_do(halos, lambda copy: copy.wait_send(), False)

    def halo_wait(halos):
        halo_do(halos, lambda copy: copy.wait_recv(), True)

    halo_start(plane)
    halo_start(down_in)
    halo_start(down)
    for where in near_z + [spot(x=x) for x in x_line]:
        pl.semaphore_signal(hello, inc=1, device_id=where, device_id_type=MESH)

    row_i = lax.broadcasted_iota(jnp.int32, (chan, chan), 0)
    col_i = lax.broadcasted_iota(jnp.int32, (chan, chan), 1)

    def natural(i):
        return (i // 4 % 4) * 32 + (i // 64) * 16 + (i // 16 % 4) * 4 + i % 4

    to_mine = jnp.where(col_i == natural(row_i), 1.0, 0.0).astype(BF16)
    to_natural = jnp.where(row_i == natural(col_i), 1.0, 0.0).astype(BF16)

    def transpose_in(slot, x, block):
        in_t[slot, :, x * ey * ez:(x + 1) * ey * ez] = lax.dot_general(
            to_mine, block.reshape(ey * ez, chan), (((1,), (1,)), ((), ())), preferred_element_type=F32
        ).astype(BF16)

    for x in range(ex):
        transpose_in(0, x, in_ref[x])

    order = [t for c in (1, 2, 0) for t in range(c, taps, 3)]

    def per_output(value):
        return jnp.sum(jnp.sum(value, axis=0), axis=0, keepdims=True)

    load_raw.wait()
    raw = raw_ref[...]
    raw_sum = per_output(raw)
    slab = core * NYC + my
    stats_w[slab, zl] = jnp.concatenate([raw_sum, per_output(raw * raw)], axis=0)
    local_mean = raw_sum / float(rows * taps)
    for u, t in enumerate(order):
        wz[zl, u] = (raw_ref[t] - local_mean).astype(BF16)
    make_faces(1, ez - 1)
    with jax.named_scope("w_hello"):
        pl.semaphore_wait(hello, len(near_z) + len(x_line))
    w1_copies = []
    for k in range(1, NZL):
        where = spot(z=zh * NZL + lax.rem(zl + k, NZL))
        w1_copies.append((wz.at[zl], wz.at[zl], where))
    gather_z = group(w1_copies, wz.at[pl.ds(0, NZL - 1)], sends.at[18], recvs.at[9])
    stats_z = group(
        [(stats_w.at[slab, zl], stats_w.at[slab, zl], where) for _, _, where in w1_copies],
        stats_w.at[slab, pl.ds(0, NZL - 1)], sends.at[19], recvs.at[10],
    )

    def view(slot, t, start, planes):
        a, b = t // 9, (t // 3) % 3
        block = shifted[slot, pl.ds(start + 2 - a, planes), 2 - b:2 - b + ey]
        return block.reshape(planes * ey * ez, chan)

    half_rows = chan // NCORE
    kinds = {1: (0, 1), 2: (1, 1), 0: (0, 2)}

    def filter_chunk(n):
        first, done, _, _ = CHUNKS[n]
        u = first
        while u < first + done:
            both = [u]
            if u + 1 < first + done and order[u + 1] % 3 == order[u] % 3:
                both.append(u + 1)
            left, slot = kinds[order[u] % 3]
            views = [view(slot, order[v], 0, ex) for v in both]
            right = jnp.concatenate(views, axis=1) if len(views) > 1 else views[0]
            product = jnp.dot(in_t[left], right, preferred_element_type=F32)
            for j, v in enumerate(both):
                for c in range(NCORE):
                    part[c, v] = product[c * half_rows:(c + 1) * half_rows, j * chan:(j + 1) * chan]
            u += len(both)
        span = pl.ds(first, done)
        return group(
            [(part.at[1 - core, span], recv_c.at[span], partner)], recv_c.at[span], sends.at[9 + n], recvs.at[n]
        )

    def xy_chunk(n, copy):
        first, done, each, slot = CHUNKS[n]
        with jax.named_scope("w_core%d" % n):
            copy.wait_recv()
        for v in range(first, first + done):
            total = part[core, v] + recv_c[v]
            for y in range(NYC):
                send_xy[y, v] = total[y * 16:(y + 1) * 16].astype(BF16)
        copies = []
        for k in range(1, NXC * NYC):
            px, py = xy_peer(k)
            copies.append((
                send_xy.at[py, pl.ds(first + px * each, each)], recv_xy.at[k - 1, pl.ds(slot, each)],
                spot(x=px, y=py),
            ))
        return group(copies, recv_xy.at[:, pl.ds(slot, each)], sends.at[12 + n], recvs.at[3 + n])

    def z_chunk(n, copy):
        first, done, each, slot = CHUNKS[n]
        with jax.named_scope("w_xy%d" % n):
            copy.wait_recv()
        span = pl.ds(slot, each)
        total = send_xy[my, pl.ds(first + mx * each, each)].astype(F32)
        for k in range(1, NXC * NYC):
            total = total + recv_xy[k - 1, span].astype(F32)
        recv_z[mz, span] = total.astype(BF16)
        return group(
            [(recv_z.at[mz, span], recv_z.at[mz, span], z_peer(k)) for k in range(1, NZR)],
            recv_z.at[pl.ds(0, NZR - 1), span], sends.at[15 + n], recvs.at[6 + n],
        )

    def shift(slot, side, amount, edge):
        depth = lax.broadcasted_iota(jnp.int32, (ey, ez, chan), 1)
        for x in range(ex + 2):
            plane = shifted[1, x, 1:ey + 1].astype(F32)
            outer = face_in[side, x].astype(F32)[:, None, :]
            shifted[slot, x, 1:ey + 1] = jnp.where(depth == edge, outer, pltpu.roll(plane, amount, 1)).astype(BF16)
        depth = lax.broadcasted_iota(jnp.int32, (ex + 2, ez, chan), 1)
        for b in range(2):
            y = (ey + 1) * b
            plane = shifted[1, :, y].astype(F32)
            outer = jnp.concatenate([
                corner_in[side, b, 0].astype(F32)[0:1], edge_in[side, b].astype(F32),
                corner_in[side, b, 1].astype(F32)[0:1],
            ], axis=0)[:, None, :]
            shifted[slot, :, y] = jnp.where(depth == edge, outer, pltpu.roll(plane, amount, 1)).astype(BF16)

    with jax.named_scope("w_halo_xy"):
        halo_wait(plane)
    with jax.named_scope("w_halo_sent"):
        halo_sent(plane)
        halo_sent(down_in)
        halo_sent(down)
    core_0 = filter_chunk(0)
    with jax.named_scope("w_halo_in"):
        halo_wait(down_in)
    depth = lax.broadcasted_iota(jnp.int32, (ey, ez, chan), 1)
    for x in range(ex):
        outer = up_in[x].astype(F32)[:, None, :]
        moved = pltpu.roll(in_ref[x].astype(F32), ez - 1, 1)
        transpose_in(1, x, jnp.where(depth == ez - 1, outer, moved).astype(BF16))
    core_1 = filter_chunk(1)
    xy_0 = xy_chunk(0, core_0)
    with jax.named_scope("w_halo_z"):
        halo_wait(down)
    halo_start(up)
    shift(2, 1, ez - 1, ez - 1)
    core_2 = filter_chunk(2)
    xy_1 = xy_chunk(1, core_1)
    with jax.named_scope("w_gather_z"):
        gather_z.wait_recv()
        stats_z.wait_recv()
    for u in range(taps):
        w_all[u, slab] = wz[:, u].astype(F32).reshape(16, chan).astype(BF16)
    core_0.wait_send()
    core_1.wait_send()
    tap_span = pl.ds(0, taps)
    gather_y = group(
        [(w_all.at[tap_span, slab], w_all.at[tap_span, slab], spot(y=y)) for y in y_line],
        w_all.at[tap_span, pl.ds(0, NYC - 1)], sends.at[9], recvs.at[11],
    )
    stats_y = group(
        [(stats_w.at[slab], stats_w.at[slab], spot(y=y)) for y in y_line],
        stats_w.at[pl.ds(0, NYC - 1)], sends.at[10], recvs.at[12],
    )
    xy_2 = xy_chunk(2, core_2)
    z_0 = z_chunk(0, xy_0)
    z_1 = z_chunk(1, xy_1)
    with jax.named_scope("w_halo_up"):
        halo_wait(up)
        halo_sent(up)
    shift(0, 0, 1, 0)
    z_2 = z_chunk(2, xy_2)
    with jax.named_scope("w_gather_y"):
        gather_y.wait_recv()
        stats_y.wait_recv()
    core_2.wait_send()
    xy_0.wait_send()
    slabs = w_all.at[tap_span, pl.ds(core * NYC, NYC)]
    gather_c = group([(slabs, slabs, partner)], slabs, sends.at[11], recvs.at[13])
    mine = stats_w.at[pl.ds(core * NYC, NYC)]
    stats_c = group([(mine, mine, partner)], mine, sends.at[12], recvs.at[14])
    with jax.named_scope("w_z"):
        z_0.wait_recv()
        z_1.wait_recv()
        z_2.wait_recv()
    grad = recv_z[0].astype(F32)
    for k in range(1, NZR):
        grad = grad + recv_z[k].astype(F32)
    pivot = stats_w[slab, 0][0:1]
    gap = [jnp.broadcast_to((stats_w[slab, q][0:1] - pivot) / float(rows * taps), (rows, chan)) for q in range(NZL)]
    gap = jnp.concatenate(gap, axis=0)
    near = []
    for first, _, each, _ in CHUNKS:
        near += [w_all[first + mx * each + j, slab].astype(F32) for j in range(each)]
    cross = grad[0] * (near[0] + gap)
    for j in range(1, SLOTS):
        cross = cross + grad[j] * (near[j] + gap)
    stats_g[flat_g] = jnp.concatenate(
        [per_output(grad), jnp.sum(cross, axis=0, keepdims=True), per_output(grad * grad), jnp.zeros((1, chan), F32)],
        axis=0,
    )
    xy_1.wait_send()
    xy_2.wait_send()
    grad_sums = group(
        [(stats_g.at[flat_g], stats_g.at[flat_g], stat_peer(k)) for k in range(1, 32)],
        stats_g.at[pl.ds(0, 31)], sends.at[13], recvs.at[15],
    )
    for j in range(SLOTS):
        owned = grad[j, 0:rows]
        for q in range(1, NZL):
            owned = jnp.where(zl == q, grad[j, q * rows:(q + 1) * rows], owned)
        full[mx, j] = owned
    gather_x = group(
        [(full.at[mx], full.at[mx], spot(x=x)) for x in x_line],
        full.at[pl.ds(0, NXC - 1)], sends.at[14], recvs.at[16],
    )

    with jax.named_scope("w_gather_c"):
        gather_c.wait_recv()
        stats_c.wait_recv()
    sums = stats_w[0, 0]
    for k in range(1, 32):
        sums = sums + stats_w[k // NZL, k % NZL]
    mean_out = sums[0:1] / fan_count
    var_out = sums[1:2] / fan_count - mean_out * mean_out
    inv_std = lax.rsqrt(var_out + var_eps)
    offset = []
    for k in range(32):
        gap = stats_w[k // NZL, k % NZL][0:1] / float(rows * taps) - mean_out
        offset.append(jnp.broadcast_to(gap, (rows, chan)))
    offset = jnp.concatenate(offset, axis=0)
    for u in range(0, taps, 2):
        pair = range(u, min(u + 2, taps))
        right = []
        for v in pair:
            value = (w_all[v].reshape(chan, chan).astype(F32) + offset) * inv_std
            right.append(value.astype(BF16))
        right = jnp.concatenate(right, axis=1) if len(right) > 1 else right[0]
        w_cat[:, u * chan:(u + len(pair)) * chan] = jnp.dot(
            to_natural, right, preferred_element_type=F32
        ).astype(BF16)
    step = 2

    def dx_step(n, carry):
        start = n * step
        left = jnp.concatenate([view(2 - t % 3, t, start, step) for t in order], axis=1)
        product = lax.dot_general(left, w_cat[...], (((1,), (1,)), ((), ())), preferred_element_type=F32)
        dx_ref[pl.ds(start, step)] = product.astype(BF16).reshape(step, ey, ez, chan)
        return carry

    with jax.named_scope("dx"):
        lax.fori_loop(0, ex // step, dx_step, 0)

    with jax.named_scope("w_grad_sums"):
        grad_sums.wait_recv()
    with jax.named_scope("w_gather_x"):
        gather_x.wait_recv()
    sum_grad, sum_cross, sum_square = (jnp.zeros((1, chan), F32) for _ in range(3))
    for k in range(32):
        one = stats_g[k]
        about = stats_w[k % NCORE * NYC + k // (NXC * NCORE), 0][0:1] / float(rows * taps) - mean_out
        sum_grad = sum_grad + one[0:1]
        sum_cross = sum_cross + (one[1:2] + about * one[0:1])
        sum_square = sum_square + one[2:3]
    sum_cross = sum_cross * inv_std
    mean_grad = sum_grad / fan_count
    mean_cross = sum_cross / fan_count
    spread = sum_square - 2.0 * mean_grad * sum_grad - 2.0 * mean_cross * sum_cross
    spread = (
        spread
        + fan_count * mean_grad * mean_grad
        + fan_count * mean_cross * mean_cross * var_out / (var_out + var_eps)
    )
    square_sum = jnp.sum(inv_std * inv_std * spread, axis=1, keepdims=True)
    scale = jnp.minimum(1.0, clip_norm * lax.rsqrt(square_sum + norm_eps))
    factor = inv_std * scale
    for first, done, each, slot in CHUNKS:
        for v in range(done):
            t = order[first + v]
            std = (raw_ref[t] - mean_out) * inv_std
            wg_ref[t] = factor * (full[v // each, slot + v % each] - mean_grad - std * mean_cross)

    with jax.named_scope("w_sends"):
        for copy in (gather_z, stats_z, gather_y, stats_y, gather_c, stats_c, z_0, z_1, z_2, grad_sums, gather_x):
            copy.wait_send()


def write_out(dx_ref, wg_ref, dx_hbm, wg_hbm, sem):
    copies = [pltpu.make_async_copy(dx_ref, dx_hbm, sem.at[0]), pltpu.make_async_copy(wg_ref, wg_hbm, sem.at[1])]
    for copy in copies:
        copy.start()
    for copy in copies:
        copy.wait()


def on_device(raw_weight, inputs, cotangent):
    rows, taps, chan = raw_weight.shape
    ex, ey, ez = inputs.shape[:3]
    dma = pltpu.SemaphoreType.DMA

    scratch = [
        pltpu.VMEM((taps, rows, chan), F32),
        pltpu.VMEM(inputs.shape, BF16),
        pltpu.VMEM((3, ex + 2, ey + 2, ez, chan), BF16),
        pltpu.VMEM((2, ex, ey, chan), BF16),
        pltpu.VMEM((2, 2, ex, chan), BF16),
        pltpu.VMEM((2, 2, 2, 2, chan), BF16),
        pltpu.VMEM((2, ex + 2, ey, chan), BF16),
        pltpu.VMEM((2, 2, ex, chan), BF16),
        pltpu.VMEM((2, 2, 2, 2, chan), BF16),
        pltpu.VMEM((ex, ey, chan), BF16),
        pltpu.VMEM((ex, ey, chan), BF16),
        pltpu.VMEM((2, chan, ex * ey * ez), BF16),
        pltpu.VMEM((NCORE, taps, chan // NCORE, chan), F32),
        pltpu.VMEM((taps, chan // NCORE, chan), F32),
        pltpu.VMEM((NYC, taps + 1, 16, chan), BF16),
        pltpu.VMEM((NXC * NYC - 1, SLOTS, 16, chan), BF16),
        pltpu.VMEM((NZR, SLOTS, 16, chan), BF16),
        pltpu.VMEM((NXC, SLOTS, rows, chan), F32),
        pltpu.VMEM((NZL, taps, rows, chan), BF16),
        pltpu.VMEM((taps + 1, 8, 16, chan), BF16),
        pltpu.VMEM((chan, taps * chan), BF16),
        pltpu.VMEM((8, NZL, 2, chan), F32),
        pltpu.VMEM((32, 4, chan), F32),
        dma((3,)), dma((20,)), dma((27,)), dma((17,)), pltpu.SemaphoreType.REGULAR,
    ]
    vmem = pl.BlockSpec(memory_space=pltpu.VMEM)
    anywhere = pl.BlockSpec(memory_space=pl.ANY)
    shapes = (
        jax.ShapeDtypeStruct(cotangent.shape, BF16),
        jax.ShapeDtypeStruct((taps, rows, chan), F32),
    )
    results = pl.pallas_call(
        kernel,
        out_shape=tuple(pltpu.VMEM(one.shape, one.dtype) for one in shapes),
        in_specs=[anywhere] * 3,
        out_specs=(vmem, vmem),
        scratch_shapes=scratch,
        compiler_params=pltpu.CompilerParams(
            collective_id=0, has_side_effects=True, vmem_limit_bytes=32 * 1024 * 1024
        ),
    )(*(
        pltpu.with_memory_space_constraint(one, pltpu.HBM)
        for one in (jnp.transpose(raw_weight, (1, 0, 2)), inputs, cotangent)
    ))
    input_grad, weight_grad = pl.pallas_call(
        write_out,
        out_shape=shapes,
        in_specs=[vmem, vmem],
        out_specs=(anywhere, anywhere),
        scratch_shapes=[dma((2,))],
    )(*(pltpu.with_memory_space_constraint(one, pltpu.VMEM) for one in results))
    return input_grad, jnp.transpose(weight_grad, (1, 0, 2))


def solution(mesh):
    in_specs = (P(("gx", "gy"), None, None), P("gx", "gy", "gz", None), P("gx", "gy", "gz", None))
    out_specs = (P("gx", "gy", "gz", None), P(("gx", "gy"), None, None))
    return jax.shard_map(
        on_device, mesh=mesh, in_specs=in_specs, out_specs=out_specs, check_vma=False
    )
```

```python
import functools

import jax
import jax.numpy as jnp
from jax import lax
from jax.experimental import pallas as pl
from jax.experimental.pallas import tpu as pltpu
from jax.sharding import PartitionSpec as P

var_eps = 1e-05
norm_eps = 1e-06
clip_norm = 600.0
F32 = jnp.float32
BF16 = jnp.bfloat16
MESH = pl.DeviceIdType.MESH
AXES = ("gx", "gy", "gz")

NCORE, NZL, NYC, NXC, NZH = 2, 4, 4, 4, 2
NZR = NZL * NZH
CHUNKS = ((0, 8, 2, 0), (8, 8, 2, 2), (16, 11, 3, 4))
SLOTS = 7


def kernel(raw_hbm, in_hbm, cot_hbm, dx_ref, wg_ref, *scratch):
    (raw_ref, in_ref, shifted, face_out, edge_out, corner_out, face_in, edge_in, corner_in, in_out, in_in, in_t,
     part, recv_c, send_xy, recv_xy, recv_z, full, wz, w_all, w_cat, stats_w, stats_g,
     load_sem, sends, halo_recv, recvs, hello) = scratch
    taps, rows, chan = raw_ref.shape
    ex, ey, ez = in_ref.shape[:3]
    fan_count = float(rows * NCORE * NZL * NYC * taps)
    count = {"gx": NCORE * NZL, "gy": NYC, "gz": NXC * NZH}
    me = {axis: lax.axis_index(axis) for axis in AXES}
    core, zl = lax.rem(me["gx"], NCORE), lax.div(me["gx"], NCORE)
    my = me["gy"]
    mx, zh = lax.rem(me["gz"], NXC), lax.div(me["gz"], NXC)
    mz = zh * NZL + zl

    def spot(c=None, x=None, y=None, z=None):
        c = core if c is None else c
        x = mx if x is None else x
        y = my if y is None else y
        z = mz if z is None else z
        return {"gx": lax.rem(z, NZL) * NCORE + c, "gy": y, "gz": lax.div(z, NZL) * NXC + x}

    partner = spot(c=1 - core)
    x_line = [lax.rem(mx + k, NXC) for k in range(1, NXC)]
    y_line = [lax.rem(my + k, NYC) for k in range(1, NYC)]

    def xy_peer(k):
        flat = lax.rem(my * NXC + mx + k, NXC * NYC)
        return lax.rem(flat, NXC), lax.div(flat, NXC)

    flat_g = (my * NXC + mx) * NCORE + core

    def stat_peer(k):
        flat = lax.rem(flat_g + k, 32)
        where = lax.div(flat, NCORE)
        return spot(c=lax.rem(flat, NCORE), x=lax.rem(where, NXC), y=lax.div(where, NXC))

    def z_peer(k):
        return spot(z=lax.rem(mz + k, NZR))

    def remote(src, dst, send_sem, recv_sem, where):
        return pltpu.make_async_remote_copy(
            src_ref=src, dst_ref=dst, send_sem=send_sem, recv_sem=recv_sem,
            device_id=where, device_id_type=MESH,
        )

    def group(copies, wholes, send_sem, recv_sem):
        for src, dst, where in copies:
            remote(src, dst, send_sem, recv_sem, where).start()
        return remote(wholes, wholes, send_sem, recv_sem, partner)

    body = pl.ds(1, ey)
    load_cot = pltpu.make_async_copy(cot_hbm, shifted.at[1, pl.ds(1, ex), body], load_sem.at[0])
    load_in = pltpu.make_async_copy(in_hbm, in_ref, load_sem.at[1])
    load_raw = pltpu.make_async_copy(raw_hbm, raw_ref, load_sem.at[2])
    load_cot.start()
    load_in.start()
    load_raw.start()

    low = {axis: me[axis] == 0 for axis in AXES}
    high = {axis: me[axis] == count[axis] - 1 for axis in AXES}
    plane_offs = [(a, b, 0) for a in (1, -1, 0) for b in (0, 1, -1) if (a, b) != (0, 0)]
    down_offs = [(a, b, -1) for a in (0, 1, -1) for b in (0, 1, -1)]
    up_offs = [(-a, -b, 1) for a, b, _ in down_offs]

    def neighbour(off):
        return {axis: lax.rem(me[axis] + count[axis] + o, count[axis]) for axis, o in zip(AXES, off)}

    def exists(off):
        ok = None
        for axis, o in zip(AXES, off):
            if o != 0:
                one = me[axis] < count[axis] - 1 if o > 0 else me[axis] > 0
                ok = one if ok is None else jnp.logical_and(ok, one)
        return ok

    barrier = pltpu.get_barrier_semaphore()
    for off in [(0, 0, 1), (0, 0, -1)] + plane_offs:

        @pl.when(exists(off))
        def _():
            pl.semaphore_signal(barrier, inc=1, device_id=neighbour(off), device_id_type=MESH)

    near_z = [spot(z=lax.rem(mz + k, NZR)) for k in (1, 2, NZR - 2, NZR - 1)]
    lines = [spot(c=c, x=x) for x in x_line for c in range(NCORE)]
    lines += [spot(c=c, y=y) for y in y_line for c in range(NCORE)]
    for where in near_z + lines:
        pl.semaphore_signal(barrier, inc=1, device_id=where, device_id_type=MESH)

    def sides(axis):
        return (me[axis] > 0).astype(jnp.int32), (me[axis] < count[axis] - 1).astype(jnp.int32)

    around = (1 + sum(sides("gx"))) * (1 + sum(sides("gy")))
    greeted = around - 1 + sum(sides("gz")) + len(near_z) + len(lines)

    tile = jnp.zeros((16, chan), BF16)
    for end, at_end in enumerate((low, high)):

        @pl.when(at_end["gx"])
        def _():
            shifted[1, (ex + 1) * end] = jnp.zeros((ey + 2, ez, chan), BF16)
            for side in range(2):
                face_in[side, (ex + 1) * end] = tile
                for b in range(2):
                    corner_in[side, b, end] = jnp.zeros((2, chan), BF16)

        @pl.when(at_end["gy"])
        def _():
            shifted[1, :, (ey + 1) * end] = jnp.zeros((ex + 2, ez, chan), BF16)
            for side in range(2):
                edge_in[side, end] = jnp.zeros((ex, chan), BF16)
                for a in range(2):
                    corner_in[side, end, a] = jnp.zeros((2, chan), BF16)

        @pl.when(at_end["gz"])
        def _():
            face_in[end] = jnp.zeros((ex + 2, ey, chan), BF16)
            edge_in[end] = jnp.zeros((2, ex, chan), BF16)
            corner_in[end] = jnp.zeros((2, 2, 2, chan), BF16)
            in_in[end] = jnp.zeros((ex, ey, chan), BF16)

    w_all[taps] = jnp.zeros((8, 16, chan), BF16)
    for y in range(NYC):
        send_xy[y, taps] = tile
    with jax.named_scope("w_cot"):
        load_cot.wait()

    def make_faces(f, z):
        firsts, lasts = [], []
        for x in range(ex):
            face = shifted[1, x + 1, 1:ey + 1].astype(F32)[:, z, :]
            face_out[f, x] = face.astype(BF16)
            firsts.append(face[0:1])
            lasts.append(face[ey - 1:ey])
        for b, edge in enumerate((firsts, lasts)):
            edge_out[f, b] = jnp.concatenate(edge, axis=0).astype(BF16)
            for a, x in enumerate((0, ex - 1)):
                corner_out[f, b, a] = jnp.concatenate([edge[x], edge[x]], axis=0).astype(BF16)

    load_in.wait()
    for x in range(ex):
        block = in_ref[x].astype(F32)
        in_out[0, x] = block[:, 0, :].astype(BF16)
        in_out[1, x] = block[:, ez - 1, :].astype(BF16)
    with jax.named_scope("w_barrier"):
        pl.semaphore_wait(barrier, greeted)

    def halo_copy(n, off, send):
        a, b, c = off
        near = {1: (ex, ey), -1: (1, 1)}
        if c == 0:
            xs = pl.ds(1, ex) if a == 0 else near[a][0]
            ys = body if b == 0 else near[b][1]
            xd = pl.ds(1, ex) if a == 0 else (0 if a > 0 else ex + 1)
            yd = body if b == 0 else (0 if b > 0 else ey + 1)
            src, dst = shifted.at[1, xs, ys], shifted.at[1, xd, yd]
        else:
            f, side = (1, 0) if c > 0 else (0, 1)
            if b == 0:
                xs = pl.ds(0, ex) if a == 0 else (ex - 1 if a > 0 else 0)
                xd = pl.ds(1, ex) if a == 0 else (0 if a > 0 else ex + 1)
                src, dst = face_out.at[f, xs], face_in.at[side, xd]
            else:
                end, ys = (1, 0) if b > 0 else (0, 1)
                src = edge_out.at[f, end] if a == 0 else corner_out.at[f, end, 1 if a > 0 else 0]
                dst = edge_in.at[side, ys] if a == 0 else corner_in.at[side, ys, 0 if a > 0 else 1]
        return remote(src, dst, sends.at[send], halo_recv.at[n], neighbour(off))

    plane = [(off, halo_copy(n, off, n)) for n, off in enumerate(plane_offs)]
    in_lo, in_hi = (
        [((0, 0, c), remote(in_out.at[f], in_in.at[1 - f], sends.at[8 + f], halo_recv.at[8 + f], neighbour((0, 0, c))))]
        for f, c in ((1, 1), (0, -1))
    )
    along = [(off, halo_copy(10 + n, off, n)) for n, off in enumerate(down_offs + up_offs)]

    def halo_do(halos, act, flip):
        for off, copy in halos:

            @pl.when(exists(tuple(-o for o in off) if flip else off))
            def _():
                act(copy)

    def halo_start(halos):
        halo_do(halos, lambda copy: copy.start(), False)

    def halo_sent(halos):
        halo_do(halos, lambda copy: copy.wait_send(), False)

    def halo_wait(halos):
        halo_do(halos, lambda copy: copy.wait_recv(), True)

    halo_start(plane)
    halo_start(in_hi)
    halo_start(in_lo)
    for where in near_z + [spot(x=x) for x in x_line]:
        pl.semaphore_signal(hello, inc=1, device_id=where, device_id_type=MESH)

    row_i = lax.broadcasted_iota(jnp.int32, (chan, chan), 0)
    col_i = lax.broadcasted_iota(jnp.int32, (chan, chan), 1)

    def natural(i):
        return (i // 4 % 4) * 32 + (i // 64) * 16 + (i // 16 % 4) * 4 + i % 4

    to_mine = jnp.where(col_i == natural(row_i), 1.0, 0.0).astype(BF16)
    to_natural = jnp.where(row_i == natural(col_i), 1.0, 0.0).astype(BF16)

    def transpose_in(slot, x, block):
        in_t[slot, :, x * ey * ez:(x + 1) * ey * ez] = lax.dot_general(
            to_mine, block.reshape(ey * ez, chan), (((1,), (1,)), ((), ())), preferred_element_type=F32
        ).astype(BF16)

    for x in range(ex):
        transpose_in(0, x, in_ref[x])

    order = [t for c in (1, 2, 0) for t in range(c, taps, 3)]

    def per_output(value):
        return jnp.sum(jnp.sum(value, axis=0), axis=0, keepdims=True)

    load_raw.wait()
    raw = raw_ref[...]
    raw_sum = per_output(raw)
    slab = core * NYC + my
    stats_w[slab, zl] = jnp.concatenate([raw_sum, per_output(raw * raw)], axis=0)
    local_mean = raw_sum / float(rows * taps)
    for u, t in enumerate(order):
        wz[zl, u] = (raw_ref[t] - local_mean).astype(BF16)
    make_faces(0, 0)
    make_faces(1, ez - 1)
    with jax.named_scope("w_hello"):
        pl.semaphore_wait(hello, len(near_z) + len(x_line))
    w1_copies = []
    for k in range(1, NZL):
        where = spot(z=zh * NZL + lax.rem(zl + k, NZL))
        w1_copies.append((wz.at[zl], wz.at[zl], where))
    gather_z = group(w1_copies, wz.at[pl.ds(0, NZL - 1)], sends.at[27], recvs.at[9])
    stats_z = group(
        [(stats_w.at[slab, zl], stats_w.at[slab, zl], where) for _, _, where in w1_copies],
        stats_w.at[slab, pl.ds(0, NZL - 1)], sends.at[28], recvs.at[10],
    )

    def view(slot, t, start, planes):
        a, b = t // 9, (t // 3) % 3
        block = shifted[slot, pl.ds(start + 2 - a, planes), 2 - b:2 - b + ey]
        return block.reshape(planes * ey * ez, chan)

    half_rows = chan // NCORE
    kinds = {1: 0, 2: 1, 0: 2}

    def filter_chunk(n):
        first, done, _, _ = CHUNKS[n]
        u = first
        while u < first + done:
            both = [u]
            if u + 1 < first + done and order[u + 1] % 3 == order[u] % 3:
                both.append(u + 1)
            views = [view(1, order[v], 0, ex) for v in both]
            right = jnp.concatenate(views, axis=1) if len(views) > 1 else views[0]
            product = jnp.dot(in_t[kinds[order[u] % 3]], right, preferred_element_type=F32)
            for j, v in enumerate(both):
                for c in range(NCORE):
                    part[c, v] = product[c * half_rows:(c + 1) * half_rows, j * chan:(j + 1) * chan]
            u += len(both)
        span = pl.ds(first, done)
        return group(
            [(part.at[1 - core, span], recv_c.at[span], partner)], recv_c.at[span], sends.at[18 + n], recvs.at[n]
        )

    def xy_chunk(n, copy):
        first, done, each, slot = CHUNKS[n]
        with jax.named_scope("w_core%d" % n):
            copy.wait_recv()
        for v in range(first, first + done):
            total = part[core, v] + recv_c[v]
            for y in range(NYC):
                send_xy[y, v] = total[y * 16:(y + 1) * 16].astype(BF16)
        copies = []
        for k in range(1, NXC * NYC):
            px, py = xy_peer(k)
            copies.append((
                send_xy.at[py, pl.ds(first + px * each, each)], recv_xy.at[k - 1, pl.ds(slot, each)],
                spot(x=px, y=py),
            ))
        return group(copies, recv_xy.at[:, pl.ds(slot, each)], sends.at[21 + n], recvs.at[3 + n])

    def z_chunk(n, copy):
        first, done, each, slot = CHUNKS[n]
        with jax.named_scope("w_xy%d" % n):
            copy.wait_recv()
        span = pl.ds(slot, each)
        total = send_xy[my, pl.ds(first + mx * each, each)].astype(F32)
        for k in range(1, NXC * NYC):
            total = total + recv_xy[k - 1, span].astype(F32)
        recv_z[mz, span] = total.astype(BF16)
        return group(
            [(recv_z.at[mz, span], recv_z.at[mz, span], z_peer(k)) for k in range(1, NZR)],
            recv_z.at[pl.ds(0, NZR - 1), span], sends.at[24 + n], recvs.at[6 + n],
        )

    def shift(slot, side, amount, edge):
        depth = lax.broadcasted_iota(jnp.int32, (ey, ez, chan), 1)
        for x in range(ex + 2):
            plane = shifted[1, x, 1:ey + 1].astype(F32)
            outer = face_in[side, x].astype(F32)[:, None, :]
            shifted[slot, x, 1:ey + 1] = jnp.where(depth == edge, outer, pltpu.roll(plane, amount, 1)).astype(BF16)
        depth = lax.broadcasted_iota(jnp.int32, (ex + 2, ez, chan), 1)
        for b in range(2):
            y = (ey + 1) * b
            plane = shifted[1, :, y].astype(F32)
            outer = jnp.concatenate([
                corner_in[side, b, 0].astype(F32)[0:1], edge_in[side, b].astype(F32),
                corner_in[side, b, 1].astype(F32)[0:1],
            ], axis=0)[:, None, :]
            shifted[slot, :, y] = jnp.where(depth == edge, outer, pltpu.roll(plane, amount, 1)).astype(BF16)

    with jax.named_scope("w_halo_xy"):
        halo_wait(plane)
    core_0 = filter_chunk(0)

    def move_in(kind, side, amount, edge):
        depth = lax.broadcasted_iota(jnp.int32, (ey, ez, chan), 1)
        for x in range(ex):
            outer = in_in[side, x].astype(F32)[:, None, :]
            moved = pltpu.roll(in_ref[x].astype(F32), amount, 1)
            transpose_in(kind, x, jnp.where(depth == edge, outer, moved).astype(BF16))

    with jax.named_scope("w_halo_hi"):
        halo_wait(in_hi)
    move_in(1, 1, ez - 1, ez - 1)
    core_1 = filter_chunk(1)
    xy_0 = xy_chunk(0, core_0)
    with jax.named_scope("w_halo_lo"):
        halo_wait(in_lo)
    halo_sent(plane)
    halo_sent(in_hi)
    halo_sent(in_lo)
    halo_start(along)
    move_in(2, 0, 1, 0)
    core_2 = filter_chunk(2)
    xy_1 = xy_chunk(1, core_1)
    xy_2 = xy_chunk(2, core_2)
    with jax.named_scope("w_gather_z"):
        gather_z.wait_recv()
        stats_z.wait_recv()
    for u in range(taps):
        w_all[u, slab] = wz[:, u].astype(F32).reshape(16, chan).astype(BF16)
    core_0.wait_send()
    core_1.wait_send()
    tap_span = pl.ds(0, taps)
    gather_y = group(
        [(w_all.at[tap_span, slab], w_all.at[tap_span, slab], spot(y=y)) for y in y_line],
        w_all.at[tap_span, pl.ds(0, NYC - 1)], sends.at[18], recvs.at[11],
    )
    stats_y = group(
        [(stats_w.at[slab], stats_w.at[slab], spot(y=y)) for y in y_line],
        stats_w.at[pl.ds(0, NYC - 1)], sends.at[19], recvs.at[12],
    )
    z_0 = z_chunk(0, xy_0)
    z_1 = z_chunk(1, xy_1)
    z_2 = z_chunk(2, xy_2)
    with jax.named_scope("w_halo_along"):
        halo_wait(along)
        halo_sent(along)
    shift(2, 1, ez - 1, ez - 1)
    shift(0, 0, 1, 0)
    with jax.named_scope("w_gather_y"):
        gather_y.wait_recv()
        stats_y.wait_recv()
    core_2.wait_send()
    xy_0.wait_send()
    slabs = w_all.at[tap_span, pl.ds(core * NYC, NYC)]
    gather_c = group([(slabs, slabs, partner)], slabs, sends.at[20], recvs.at[13])
    mine = stats_w.at[pl.ds(core * NYC, NYC)]
    stats_c = group([(mine, mine, partner)], mine, sends.at[21], recvs.at[14])
    with jax.named_scope("w_z"):
        z_0.wait_recv()
        z_1.wait_recv()
        z_2.wait_recv()
    grad = recv_z[0].astype(F32)
    for k in range(1, NZR):
        grad = grad + recv_z[k].astype(F32)
    pivot = stats_w[slab, 0][0:1]
    gap = [jnp.broadcast_to((stats_w[slab, q][0:1] - pivot) / float(rows * taps), (rows, chan)) for q in range(NZL)]
    gap = jnp.concatenate(gap, axis=0)
    near = []
    for first, _, each, _ in CHUNKS:
        near += [w_all[first + mx * each + j, slab].astype(F32) for j in range(each)]
    cross = grad[0] * (near[0] + gap)
    for j in range(1, SLOTS):
        cross = cross + grad[j] * (near[j] + gap)
    stats_g[flat_g] = jnp.concatenate(
        [per_output(grad), jnp.sum(cross, axis=0, keepdims=True), per_output(grad * grad), jnp.zeros((1, chan), F32)],
        axis=0,
    )
    xy_1.wait_send()
    xy_2.wait_send()
    grad_sums = group(
        [(stats_g.at[flat_g], stats_g.at[flat_g], stat_peer(k)) for k in range(1, 32)],
        stats_g.at[pl.ds(0, 31)], sends.at[22], recvs.at[15],
    )
    for j in range(SLOTS):
        owned = grad[j, 0:rows]
        for q in range(1, NZL):
            owned = jnp.where(zl == q, grad[j, q * rows:(q + 1) * rows], owned)
        full[mx, j] = owned
    gather_x = group(
        [(full.at[mx], full.at[mx], spot(x=x)) for x in x_line],
        full.at[pl.ds(0, NXC - 1)], sends.at[23], recvs.at[16],
    )

    with jax.named_scope("w_gather_c"):
        gather_c.wait_recv()
        stats_c.wait_recv()
    sums = stats_w[0, 0]
    for k in range(1, 32):
        sums = sums + stats_w[k // NZL, k % NZL]
    mean_out = sums[0:1] / fan_count
    var_out = sums[1:2] / fan_count - mean_out * mean_out
    inv_std = lax.rsqrt(var_out + var_eps)
    offset = []
    for k in range(32):
        gap = stats_w[k // NZL, k % NZL][0:1] / float(rows * taps) - mean_out
        offset.append(jnp.broadcast_to(gap, (rows, chan)))
    offset = jnp.concatenate(offset, axis=0)
    for u in range(0, taps, 2):
        pair = range(u, min(u + 2, taps))
        right = []
        for v in pair:
            value = (w_all[v].reshape(chan, chan).astype(F32) + offset) * inv_std
            right.append(value.astype(BF16))
        right = jnp.concatenate(right, axis=1) if len(right) > 1 else right[0]
        w_cat[:, u * chan:(u + len(pair)) * chan] = jnp.dot(
            to_natural, right, preferred_element_type=F32
        ).astype(BF16)
    step = 2

    def dx_step(n, carry):
        start = n * step
        left = jnp.concatenate([view(2 - t % 3, t, start, step) for t in order], axis=1)
        product = lax.dot_general(left, w_cat[...], (((1,), (1,)), ((), ())), preferred_element_type=F32)
        dx_ref[pl.ds(start, step)] = product.astype(BF16).reshape(step, ey, ez, chan)
        return carry

    with jax.named_scope("dx"):
        lax.fori_loop(0, ex // step, dx_step, 0)

    with jax.named_scope("w_grad_sums"):
        grad_sums.wait_recv()
    with jax.named_scope("w_gather_x"):
        gather_x.wait_recv()
    sum_grad, sum_cross, sum_square = (jnp.zeros((1, chan), F32) for _ in range(3))
    for k in range(32):
        one = stats_g[k]
        about = stats_w[k % NCORE * NYC + k // (NXC * NCORE), 0][0:1] / float(rows * taps) - mean_out
        sum_grad = sum_grad + one[0:1]
        sum_cross = sum_cross + (one[1:2] + about * one[0:1])
        sum_square = sum_square + one[2:3]
    sum_cross = sum_cross * inv_std
    mean_grad = sum_grad / fan_count
    mean_cross = sum_cross / fan_count
    spread = sum_square - 2.0 * mean_grad * sum_grad - 2.0 * mean_cross * sum_cross
    spread = (
        spread
        + fan_count * mean_grad * mean_grad
        + fan_count * mean_cross * mean_cross * var_out / (var_out + var_eps)
    )
    square_sum = jnp.sum(inv_std * inv_std * spread, axis=1, keepdims=True)
    scale = jnp.minimum(1.0, clip_norm * lax.rsqrt(square_sum + norm_eps))
    factor = inv_std * scale
    for first, done, each, slot in CHUNKS:
        for v in range(done):
            t = order[first + v]
            std = (raw_ref[t] - mean_out) * inv_std
            wg_ref[t] = factor * (full[v // each, slot + v % each] - mean_grad - std * mean_cross)

    with jax.named_scope("w_sends"):
        for copy in (gather_z, stats_z, gather_y, stats_y, gather_c, stats_c, z_0, z_1, z_2, grad_sums, gather_x):
            copy.wait_send()


def write_out(dx_ref, wg_ref, dx_hbm, wg_hbm, sem):
    copies = [pltpu.make_async_copy(dx_ref, dx_hbm, sem.at[0]), pltpu.make_async_copy(wg_ref, wg_hbm, sem.at[1])]
    for copy in copies:
        copy.start()
    for copy in copies:
        copy.wait()


def on_device(raw_weight, inputs, cotangent):
    rows, taps, chan = raw_weight.shape
    ex, ey, ez = inputs.shape[:3]
    dma = pltpu.SemaphoreType.DMA

    scratch = [
        pltpu.VMEM((taps, rows, chan), F32),
        pltpu.VMEM(inputs.shape, BF16),
        pltpu.VMEM((3, ex + 2, ey + 2, ez, chan), BF16),
        pltpu.VMEM((2, ex, ey, chan), BF16),
        pltpu.VMEM((2, 2, ex, chan), BF16),
        pltpu.VMEM((2, 2, 2, 2, chan), BF16),
        pltpu.VMEM((2, ex + 2, ey, chan), BF16),
        pltpu.VMEM((2, 2, ex, chan), BF16),
        pltpu.VMEM((2, 2, 2, 2, chan), BF16),
        pltpu.VMEM((2, ex, ey, chan), BF16),
        pltpu.VMEM((2, ex, ey, chan), BF16),
        pltpu.VMEM((3, chan, ex * ey * ez), BF16),
        pltpu.VMEM((NCORE, taps, chan // NCORE, chan), F32),
        pltpu.VMEM((taps, chan // NCORE, chan), F32),
        pltpu.VMEM((NYC, taps + 1, 16, chan), BF16),
        pltpu.VMEM((NXC * NYC - 1, SLOTS, 16, chan), BF16),
        pltpu.VMEM((NZR, SLOTS, 16, chan), BF16),
        pltpu.VMEM((NXC, SLOTS, rows, chan), F32),
        pltpu.VMEM((NZL, taps, rows, chan), BF16),
        pltpu.VMEM((taps + 1, 8, 16, chan), BF16),
        pltpu.VMEM((chan, taps * chan), BF16),
        pltpu.VMEM((8, NZL, 2, chan), F32),
        pltpu.VMEM((32, 4, chan), F32),
        dma((3,)), dma((29,)), dma((28,)), dma((17,)), pltpu.SemaphoreType.REGULAR,
    ]
    vmem = pl.BlockSpec(memory_space=pltpu.VMEM)
    anywhere = pl.BlockSpec(memory_space=pl.ANY)
    shapes = (
        jax.ShapeDtypeStruct(cotangent.shape, BF16),
        jax.ShapeDtypeStruct((taps, rows, chan), F32),
    )
    results = pl.pallas_call(
        kernel,
        out_shape=tuple(pltpu.VMEM(one.shape, one.dtype) for one in shapes),
        in_specs=[anywhere] * 3,
        out_specs=(vmem, vmem),
        scratch_shapes=scratch,
        compiler_params=pltpu.CompilerParams(
            collective_id=0, has_side_effects=True, vmem_limit_bytes=32 * 1024 * 1024
        ),
    )(*(
        pltpu.with_memory_space_constraint(one, pltpu.HBM)
        for one in (jnp.transpose(raw_weight, (1, 0, 2)), inputs, cotangent)
    ))
    input_grad, weight_grad = pl.pallas_call(
        write_out,
        out_shape=shapes,
        in_specs=[vmem, vmem],
        out_specs=(anywhere, anywhere),
        scratch_shapes=[dma((2,))],
    )(*(pltpu.with_memory_space_constraint(one, pltpu.VMEM) for one in results))
    return input_grad, jnp.transpose(weight_grad, (1, 0, 2))


def solution(mesh):
    in_specs = (P(("gx", "gy"), None, None), P("gx", "gy", "gz", None), P("gx", "gy", "gz", None))
    out_specs = (P("gx", "gy", "gz", None), P(("gx", "gy"), None, None))
    return jax.shard_map(
        on_device, mesh=mesh, in_specs=in_specs, out_specs=out_specs, check_vma=False
    )
```

```python
import functools

import jax
import jax.numpy as jnp
from jax import lax
from jax.experimental import pallas as pl
from jax.experimental.pallas import tpu as pltpu
from jax.sharding import PartitionSpec as P

var_eps = 1e-05
norm_eps = 1e-06
clip_norm = 600.0
F32 = jnp.float32
BF16 = jnp.bfloat16
MESH = pl.DeviceIdType.MESH
AXES = ("gx", "gy", "gz")

NCORE, NZL, NYC, NXC, NZH = 2, 4, 4, 4, 2
NZR = NZL * NZH
CHUNKS = ((0, 8, 2, 0), (8, 8, 2, 2), (16, 11, 3, 4))
SLOTS = 7
W_SPLIT = 9


def kernel(raw_hbm, in_hbm, cot_hbm, dx_ref, wg_ref, *scratch):
    (raw_ref, in_ref, shifted, halo_x, halo_y, along_out, along_in, in_out, in_in, in_t, edge_y, edge_t, rim, rim_view,
     part, recv_c, send_xy, recv_xy, recv_z, full, wz, w_all, w_cat, dx_acc, stats_w, stats_g,
     load_sem, sends, halo_recv, recvs, hello) = scratch
    taps, rows, chan = raw_ref.shape
    ex, ey, ez = in_ref.shape[:3]
    fan_count = float(rows * NCORE * NZL * NYC * taps)
    count = {"gx": NCORE * NZL, "gy": NYC, "gz": NXC * NZH}
    me = {axis: lax.axis_index(axis) for axis in AXES}
    core, zl = lax.rem(me["gx"], NCORE), lax.div(me["gx"], NCORE)
    my = me["gy"]
    mx, zh = lax.rem(me["gz"], NXC), lax.div(me["gz"], NXC)
    mz = zh * NZL + zl

    def spot(c=None, x=None, y=None, z=None):
        c = core if c is None else c
        x = mx if x is None else x
        y = my if y is None else y
        z = mz if z is None else z
        return {"gx": lax.rem(z, NZL) * NCORE + c, "gy": y, "gz": lax.div(z, NZL) * NXC + x}

    partner = spot(c=1 - core)
    x_line = [lax.rem(mx + k, NXC) for k in range(1, NXC)]
    y_line = [lax.rem(my + k, NYC) for k in range(1, NYC)]

    def xy_peer(k):
        flat = lax.rem(my * NXC + mx + k, NXC * NYC)
        return lax.rem(flat, NXC), lax.div(flat, NXC)

    flat_g = (my * NXC + mx) * NCORE + core

    def stat_peer(k):
        flat = lax.rem(flat_g + k, 32)
        where = lax.div(flat, NCORE)
        return spot(c=lax.rem(flat, NCORE), x=lax.rem(where, NXC), y=lax.div(where, NXC))

    def z_peer(k):
        return spot(z=lax.rem(mz + k, NZR))

    def remote(src, dst, send_sem, recv_sem, where):
        return pltpu.make_async_remote_copy(
            src_ref=src, dst_ref=dst, send_sem=send_sem, recv_sem=recv_sem,
            device_id=where, device_id_type=MESH,
        )

    def group(copies, wholes, send_sem, recv_sem):
        for src, dst, where in copies:
            remote(src, dst, send_sem, recv_sem, where).start()
        return remote(wholes, wholes, send_sem, recv_sem, partner)

    body = pl.ds(1, ey)
    load_cot = pltpu.make_async_copy(cot_hbm, shifted.at[1, pl.ds(1, ex), body], load_sem.at[0])
    load_in = pltpu.make_async_copy(in_hbm, in_ref, load_sem.at[1])
    load_raw = pltpu.make_async_copy(raw_hbm, raw_ref, load_sem.at[2])
    load_cot.start()
    load_in.start()
    load_raw.start()

    low = {axis: me[axis] == 0 for axis in AXES}
    high = {axis: me[axis] == count[axis] - 1 for axis in AXES}
    plane_offs = [(a, b, 0) for a in (1, -1, 0) for b in (0, 1, -1) if (a, b) != (0, 0)]

    def neighbour(off):
        return {axis: lax.rem(me[axis] + count[axis] + o, count[axis]) for axis, o in zip(AXES, off)}

    def exists(off):
        ok = None
        for axis, o in zip(AXES, off):
            if o != 0:
                one = me[axis] < count[axis] - 1 if o > 0 else me[axis] > 0
                ok = one if ok is None else jnp.logical_and(ok, one)
        return ok

    barrier = pltpu.get_barrier_semaphore()
    for off in [(0, 0, 1), (0, 0, -1)] + plane_offs:

        @pl.when(exists(off))
        def _():
            pl.semaphore_signal(barrier, inc=1, device_id=neighbour(off), device_id_type=MESH)

    near_z = [spot(z=lax.rem(mz + k, NZR)) for k in (1, 2, NZR - 2, NZR - 1)]
    lines = [spot(c=c, x=x) for x in x_line for c in range(NCORE)]
    lines += [spot(c=c, y=y) for y in y_line for c in range(NCORE)]
    for where in near_z + lines:
        pl.semaphore_signal(barrier, inc=1, device_id=where, device_id_type=MESH)

    line_end = jnp.logical_or(zl == 0, zl == NZL - 1)

    @pl.when(line_end)
    def _():
        where = spot(z=zh * NZL + NZL - 1 - zl)
        pl.semaphore_signal(barrier, inc=1, device_id=where, device_id_type=MESH)

    def sides(axis):
        return (me[axis] > 0).astype(jnp.int32), (me[axis] < count[axis] - 1).astype(jnp.int32)

    around = (1 + sum(sides("gx"))) * (1 + sum(sides("gy")))
    greeted = around - 1 + sum(sides("gz")) + len(near_z) + len(lines) + line_end.astype(jnp.int32)

    tile = jnp.zeros((16, chan), BF16)
    for end, at_end in enumerate((low, high)):
        shifted[1, (ex + 1) * end] = jnp.zeros((ey + 2, ez, chan), BF16)
        shifted[1, :, (ey + 1) * end] = jnp.zeros((ex + 2, ez, chan), BF16)
        for side in range(2):
            halo_y[side, (ex + 1) * end] = tile

        @pl.when(at_end["gx"])
        def _():
            halo_x[end] = jnp.zeros((ey + 2, ez, chan), BF16)

        @pl.when(at_end["gy"])
        def _():
            for side in range(2):
                halo_x[side, (ey + 1) * end] = tile
            halo_y[end, 1:ex + 1] = jnp.zeros((ex, ez, chan), BF16)

        @pl.when(at_end["gz"])
        def _():
            in_in[end] = jnp.zeros((ex, ey, chan), BF16)
            along_in[end] = jnp.zeros((ex + 4, ey, chan), BF16)

    w_all[taps] = jnp.zeros((8, 16, chan), BF16)
    for y in range(NYC):
        send_xy[y, taps] = tile
    with jax.named_scope("w_cot"):
        load_cot.wait()

    load_in.wait()
    for x in range(ex):
        block = in_ref[x].astype(F32)
        in_out[0, x] = block[:, 0, :].astype(BF16)
        in_out[1, x] = block[:, ez - 1, :].astype(BF16)
    order = [t for c in (1, 2, 0) for t in range(c, taps, 3)]

    def per_output(value):
        return jnp.sum(jnp.sum(value, axis=0), axis=0, keepdims=True)

    load_raw.wait()
    raw = raw_ref[...]
    raw_sum = per_output(raw)
    slab = core * NYC + my
    stats_w[slab, zl] = jnp.concatenate([raw_sum, per_output(raw * raw)], axis=0)
    local_mean = raw_sum / float(rows * taps)
    for u, t in enumerate(order):
        wz[zl, u] = (raw_ref[t] - local_mean).astype(BF16)
    row_i = lax.broadcasted_iota(jnp.int32, (chan, chan), 0)
    col_i = lax.broadcasted_iota(jnp.int32, (chan, chan), 1)

    def natural(i):
        return (i // 4 % 4) * 32 + (i // 64) * 16 + (i // 16 % 4) * 4 + i % 4

    to_mine = jnp.where(col_i == natural(row_i), 1.0, 0.0).astype(BF16)
    to_natural = jnp.where(row_i == natural(col_i), 1.0, 0.0).astype(BF16)

    def transposed(block):
        return lax.dot_general(
            to_mine, block, (((1,), (1,)), ((), ())), preferred_element_type=F32
        ).astype(BF16)

    depth = lax.broadcasted_iota(jnp.int32, (ey, ez, chan), 1)
    for kind in range(3):
        ends = [[], []]
        for x in range(ex):
            block = in_ref[x]
            if kind:
                moved = pltpu.roll(block.astype(F32), ez - 1 if kind == 1 else 1, 1)
                block = jnp.where(depth == (ez - 1 if kind == 1 else 0), 0.0, moved).astype(BF16)
            in_t[kind, :, x * ey * ez:(x + 1) * ey * ez] = transposed(block.reshape(ey * ez, chan))
            ends[0].append(block[0])
            ends[1].append(block[ey - 1])
        for side in range(2):
            edge_y[side, kind] = transposed(jnp.concatenate(ends[side], axis=0))
    with jax.named_scope("w_barrier"):
        pl.semaphore_wait(barrier, greeted)

    def plane_copy(n, off):
        a, b, _ = off
        near = {1: (ex, ey), -1: (1, 1)}
        side = {1: 0, -1: 1}
        if b == 0:
            src, dst = shifted.at[1, near[a][0], body], halo_x.at[side[a], body]
        elif a == 0:
            src, dst = shifted.at[1, pl.ds(1, ex), near[b][1]], halo_y.at[side[b], pl.ds(1, ex)]
        else:
            src, dst = shifted.at[1, near[a][0], near[b][1]], halo_x.at[side[a], 0 if b > 0 else ey + 1]
        return remote(src, dst, sends.at[n], halo_recv.at[n], neighbour(off))

    def z_copies(n, source, target):
        pairs = []
        for f, off in ((1, (0, 0, 1)), (0, (0, 0, -1))):
            copy = remote(source.at[f], target.at[1 - f], sends.at[n + f], halo_recv.at[n + f], neighbour(off))
            pairs.append([(off, copy)])
        return pairs

    plane = [(off, plane_copy(n, off)) for n, off in enumerate(plane_offs)]
    in_lo, in_hi = z_copies(8, in_out, in_in)
    along = sum(z_copies(10, along_out, along_in), [])

    def halo_do(halos, act, flip):
        for off, copy in halos:

            @pl.when(exists(tuple(-o for o in off) if flip else off))
            def _():
                act(copy)

    def halo_start(halos):
        halo_do(halos, lambda copy: copy.start(), False)

    def halo_sent(halos):
        halo_do(halos, lambda copy: copy.wait_send(), False)

    def halo_wait(halos):
        halo_do(halos, lambda copy: copy.wait_recv(), True)

    halo_start(plane)
    halo_start(in_hi)
    halo_start(in_lo)
    w1_copies = []
    for k in range(1, NZL):
        where = spot(z=zh * NZL + lax.rem(zl + k, NZL))
        w1_copies.append((wz.at[zl], wz.at[zl], where))
    gather_z = group(w1_copies, wz.at[pl.ds(0, NZL - 1)], sends.at[21], recvs.at[9])
    stats_z = group(
        [(stats_w.at[slab, zl], stats_w.at[slab, zl], where) for _, _, where in w1_copies],
        stats_w.at[slab, pl.ds(0, NZL - 1)], sends.at[22], recvs.at[10],
    )
    for where in near_z + [spot(x=x) for x in x_line]:
        pl.semaphore_signal(hello, inc=1, device_id=where, device_id_type=MESH)

    def view(slot, t, start, planes):
        a, b = t // 9, (t // 3) % 3
        block = shifted[slot, pl.ds(start + 2 - a, planes), 2 - b:2 - b + ey]
        return block.reshape(planes * ey * ez, chan)

    half_rows = chan // NCORE
    kinds = {1: 0, 2: 1, 0: 2}

    def products(first, last, left, right_of):
        u = first
        while u < last:
            both = [u]
            if u + 1 < last and order[u + 1] % 3 == order[u] % 3:
                both.append(u + 1)
            views = [right_of(order[v]) for v in both]
            right = jnp.concatenate(views, axis=1) if len(views) > 1 else views[0]
            product = jnp.dot(left(order[u]), right, preferred_element_type=F32)
            for j, v in enumerate(both):
                for c in range(NCORE):
                    yield c, v, product[c * half_rows:(c + 1) * half_rows, j * chan:(j + 1) * chan]
            u += len(both)

    def filter_main(first, last):
        for c, v, value in products(first, last, lambda t: in_t[kinds[t % 3]], lambda t: view(1, t, 0, ex)):
            part[c, v] = value

    where_is = {t: v for v, t in enumerate(order)}
    tap_c = (1, 2, 0)

    def filter_side(left, rights, taps_of):
        product = jnp.dot(left, jnp.concatenate(rights, axis=1), preferred_element_type=F32)
        for kind in range(3):
            for j in range(3):
                v = where_is[taps_of(j) + tap_c[kind]]
                for c in range(NCORE):
                    low_row = kind * chan + c * half_rows
                    part[c, v] = part[c, v] + product[low_row:low_row + half_rows, j * chan:(j + 1) * chan]

    def filter_plane():
        for side, a, x in ((1, 0, ex - 1), (0, 2, 0)):
            left = in_t[:, :, x * ey * ez:(x + 1) * ey * ez].reshape(3 * chan, ey * ez)
            rights = [halo_x[side, 2 - b:2 - b + ey].reshape(ey * ez, chan) for b in range(3)]
            filter_side(left, rights, lambda b: a * 9 + b * 3)
        for side, b in ((1, 0), (0, 2)):
            left = edge_y[side].reshape(3 * chan, ex * ez)
            rights = [halo_y[side, 2 - a:2 - a + ex].reshape(ex * ez, chan) for a in range(3)]
            filter_side(left, rights, lambda a: a * 9 + b * 3)

    def fill_plane():
        for side in range(2):
            shifted[1, (ex + 1) * side] = halo_x[side]
            shifted[1, 1:ex + 1, (ey + 1) * side] = halo_y[side, 1:ex + 1]

    def make_rim():
        for x in range(ex + 2):
            plane = shifted[1, x].astype(F32)
            for side, z in enumerate((0, ez - 1)):
                rim[side, x, 0:ey + 2] = plane[:, z, :]
        for side in range(2):
            for b in range(3):
                rim_view[side, b] = rim[side, :, 2 - b:2 - b + ey].astype(BF16)
            along_out[side, 0:ex + 2] = rim_view[side, 1]
            for b in range(2):
                ends = jnp.concatenate([rim[side, :, (ey + 1) * b], jnp.zeros((ey - ex - 2, chan), F32)], axis=0)
                along_out[side, ex + 2 + b] = ends.astype(BF16)

    def filter_rim(side, first, last):
        edge_t[side] = transposed(in_in[side].reshape(ex * ey, chan))

        def rim_of(t):
            a, b = t // 9, (t // 3) % 3
            return rim_view[side, b, 2 - a:2 - a + ex].reshape(ex * ey, chan)

        for c, v, value in products(first, last, lambda t: edge_t[side], rim_of):
            part[c, v] = part[c, v] + value

    def core_chunk(n):
        first, done, _, _ = CHUNKS[n]
        span = pl.ds(first, done)
        return group(
            [(part.at[1 - core, span], recv_c.at[span], partner)], recv_c.at[span], sends.at[12 + n], recvs.at[n]
        )

    def xy_chunk(n, copy):
        first, done, each, slot = CHUNKS[n]
        with jax.named_scope("w_core%d" % n):
            copy.wait_recv()
        for v in range(first, first + done):
            total = part[core, v] + recv_c[v]
            for y in range(NYC):
                send_xy[y, v] = total[y * 16:(y + 1) * 16].astype(BF16)
        copies = []
        for k in range(1, NXC * NYC):
            px, py = xy_peer(k)
            copies.append((
                send_xy.at[py, pl.ds(first + px * each, each)], recv_xy.at[k - 1, pl.ds(slot, each)],
                spot(x=px, y=py),
            ))
        return group(copies, recv_xy.at[:, pl.ds(slot, each)], sends.at[15 + n], recvs.at[3 + n])

    def z_chunk(n, copy):
        first, done, each, slot = CHUNKS[n]
        with jax.named_scope("w_xy%d" % n):
            copy.wait_recv()
        span = pl.ds(slot, each)
        total = send_xy[my, pl.ds(first + mx * each, each)].astype(F32)
        for k in range(1, NXC * NYC):
            total = total + recv_xy[k - 1, span].astype(F32)
        recv_z[mz, span] = total.astype(BF16)
        return group(
            [(recv_z.at[mz, span], recv_z.at[mz, span], z_peer(k)) for k in range(1, NZR)],
            recv_z.at[pl.ds(0, NZR - 1), span], sends.at[18 + n], recvs.at[6 + n],
        )

    def shift(slot, side, amount, edge):
        depth = lax.broadcasted_iota(jnp.int32, (ey, ez, chan), 1)
        for x in range(ex + 2):
            plane = shifted[1, x, 1:ey + 1].astype(F32)
            outer = along_in[side, x].astype(F32)[:, None, :]
            shifted[slot, x, 1:ey + 1] = jnp.where(depth == edge, outer, pltpu.roll(plane, amount, 1)).astype(BF16)
        depth = lax.broadcasted_iota(jnp.int32, (ex + 2, ez, chan), 1)
        for b in range(2):
            y = (ey + 1) * b
            plane = shifted[1, :, y].astype(F32)
            outer = along_in[side, ex + 2 + b].astype(F32)[0:ex + 2][:, None, :]
            shifted[slot, :, y] = jnp.where(depth == edge, outer, pltpu.roll(plane, amount, 1)).astype(BF16)

    filter_main(0, taps)
    with jax.named_scope("w_halo_xy"):
        halo_wait(plane)
    filter_plane()
    core_0 = core_chunk(0)
    fill_plane()
    make_rim()
    with jax.named_scope("w_halo_hi"):
        halo_wait(in_hi)
    filter_rim(1, 9, 18)
    core_1 = core_chunk(1)
    with jax.named_scope("w_halo_lo"):
        halo_wait(in_lo)
    filter_rim(0, 18, 27)
    core_2 = core_chunk(2)
    with jax.named_scope("w_hello"):
        pl.semaphore_wait(hello, len(near_z) + len(x_line))
    xy_0 = xy_chunk(0, core_0)
    with jax.named_scope("w_gather_z"):
        gather_z.wait_recv()
        stats_z.wait_recv()
    for u in range(taps):
        w_all[u, slab] = wz[:, u].astype(F32).reshape(16, chan).astype(BF16)

    def gather_part(first, last, send, recv):
        span = pl.ds(first, last - first)
        return group(
            [(w_all.at[span, slab], w_all.at[span, slab], spot(y=y)) for y in y_line],
            w_all.at[span, pl.ds(0, NYC - 1)], sends.at[send], recvs.at[recv],
        )

    def share_part(first, last, send, recv):
        slabs = w_all.at[pl.ds(first, last - first), pl.ds(core * NYC, NYC)]
        return group([(slabs, slabs, partner)], slabs, sends.at[send], recvs.at[recv])

    gather_y = gather_part(0, W_SPLIT, 23, 11)
    stats_y = group(
        [(stats_w.at[slab], stats_w.at[slab], spot(y=y)) for y in y_line],
        stats_w.at[pl.ds(0, NYC - 1)], sends.at[24], recvs.at[12],
    )
    xy_1 = xy_chunk(1, core_1)
    xy_2 = xy_chunk(2, core_2)
    gather_y2 = gather_part(W_SPLIT, taps, 25, 17)
    halo_start(along)
    for halos in (plane, in_hi, in_lo):
        halo_sent(halos)
    z_0 = z_chunk(0, xy_0)
    with jax.named_scope("w_gather_y"):
        gather_y.wait_recv()
        stats_y.wait_recv()
    core_0.wait_send()
    core_1.wait_send()
    gather_c = share_part(0, W_SPLIT, 12, 13)
    mine = stats_w.at[pl.ds(core * NYC, NYC)]
    stats_c = group([(mine, mine, partner)], mine, sends.at[13], recvs.at[14])
    z_1 = z_chunk(1, xy_1)
    z_2 = z_chunk(2, xy_2)

    with jax.named_scope("w_gather_c"):
        gather_c.wait_recv()
        stats_c.wait_recv()
    sums = stats_w[0, 0]
    for k in range(1, 32):
        sums = sums + stats_w[k // NZL, k % NZL]
    mean_out = sums[0:1] / fan_count
    var_out = sums[1:2] / fan_count - mean_out * mean_out
    inv_std = lax.rsqrt(var_out + var_eps)
    offset = []
    for k in range(32):
        gap = stats_w[k // NZL, k % NZL][0:1] / float(rows * taps) - mean_out
        offset.append(jnp.broadcast_to(gap, (rows, chan)))
    offset = jnp.concatenate(offset, axis=0)

    def standardize(first, last):
        for u in range(first, last, 2):
            pair = range(u, min(u + 2, last))
            right = []
            for v in pair:
                value = (w_all[v].reshape(chan, chan).astype(F32) + offset) * inv_std
                right.append(value.astype(BF16))
            right = jnp.concatenate(right, axis=1) if len(right) > 1 else right[0]
            w_cat[:, u * chan:(u + len(pair)) * chan] = jnp.dot(
                to_natural, right, preferred_element_type=F32
            ).astype(BF16)

    def dx_steps(first, last, step, finish):
        def dx_step(n, carry):
            start = n * step
            left = jnp.concatenate([view(2 - t % 3, t, start, step) for t in order[first:last]], axis=1)
            product = lax.dot_general(
                left, w_cat[:, first * chan:last * chan], (((1,), (1,)), ((), ())), preferred_element_type=F32
            )
            finish(pl.ds(start, step), product.reshape(step, ey, ez, chan))
            return carry

        lax.fori_loop(0, ex // step, dx_step, 0)

    def keep(span, value):
        dx_acc[span] = value

    def finish(span, value):
        dx_ref[span] = (value + dx_acc[span]).astype(BF16)

    standardize(0, W_SPLIT)
    with jax.named_scope("dxa"):
        dx_steps(0, W_SPLIT, 2, keep)
    with jax.named_scope("w_gather_y2"):
        gather_y2.wait_recv()
    core_2.wait_send()
    gather_c2 = share_part(W_SPLIT, taps, 14, 18)

    with jax.named_scope("w_z"):
        z_0.wait_recv()
        z_1.wait_recv()
        z_2.wait_recv()
    grad = recv_z[0].astype(F32)
    for k in range(1, NZR):
        grad = grad + recv_z[k].astype(F32)
    pivot = stats_w[slab, 0][0:1]
    gap = [jnp.broadcast_to((stats_w[slab, q][0:1] - pivot) / float(rows * taps), (rows, chan)) for q in range(NZL)]
    gap = jnp.concatenate(gap, axis=0)
    near = []
    for first, _, each, _ in CHUNKS:
        near += [w_all[first + mx * each + j, slab].astype(F32) for j in range(each)]
    cross = grad[0] * (near[0] + gap)
    for j in range(1, SLOTS):
        cross = cross + grad[j] * (near[j] + gap)
    stats_g[flat_g] = jnp.concatenate(
        [per_output(grad), jnp.sum(cross, axis=0, keepdims=True), per_output(grad * grad), jnp.zeros((1, chan), F32)],
        axis=0,
    )
    xy_0.wait_send()
    xy_1.wait_send()
    grad_sums = group(
        [(stats_g.at[flat_g], stats_g.at[flat_g], stat_peer(k)) for k in range(1, 32)],
        stats_g.at[pl.ds(0, 31)], sends.at[15], recvs.at[15],
    )
    for j in range(SLOTS):
        owned = grad[j, 0:rows]
        for q in range(1, NZL):
            owned = jnp.where(zl == q, grad[j, q * rows:(q + 1) * rows], owned)
        full[mx, j] = owned
    gather_x = group(
        [(full.at[mx], full.at[mx], spot(x=x)) for x in x_line],
        full.at[pl.ds(0, NXC - 1)], sends.at[16], recvs.at[16],
    )

    with jax.named_scope("w_halo_along"):
        halo_wait(along)
        halo_sent(along)
    shift(2, 1, ez - 1, ez - 1)
    shift(0, 0, 1, 0)
    with jax.named_scope("w_gather_c2"):
        gather_c2.wait_recv()
    standardize(W_SPLIT, taps)
    with jax.named_scope("dxb"):
        dx_steps(W_SPLIT, taps, 2, finish)

    with jax.named_scope("w_grad_sums"):
        grad_sums.wait_recv()
    with jax.named_scope("w_gather_x"):
        gather_x.wait_recv()
    sum_grad, sum_cross, sum_square = (jnp.zeros((1, chan), F32) for _ in range(3))
    for k in range(32):
        one = stats_g[k]
        about = stats_w[k % NCORE * NYC + k // (NXC * NCORE), 0][0:1] / float(rows * taps) - mean_out
        sum_grad = sum_grad + one[0:1]
        sum_cross = sum_cross + (one[1:2] + about * one[0:1])
        sum_square = sum_square + one[2:3]
    sum_cross = sum_cross * inv_std
    mean_grad = sum_grad / fan_count
    mean_cross = sum_cross / fan_count
    spread = sum_square - 2.0 * mean_grad * sum_grad - 2.0 * mean_cross * sum_cross
    spread = (
        spread
        + fan_count * mean_grad * mean_grad
        + fan_count * mean_cross * mean_cross * var_out / (var_out + var_eps)
    )
    square_sum = jnp.sum(inv_std * inv_std * spread, axis=1, keepdims=True)
    scale = jnp.minimum(1.0, clip_norm * lax.rsqrt(square_sum + norm_eps))
    factor = inv_std * scale
    for first, done, each, slot in CHUNKS:
        for v in range(done):
            t = order[first + v]
            std = (raw_ref[t] - mean_out) * inv_std
            wg_ref[t] = factor * (full[v // each, slot + v % each] - mean_grad - std * mean_cross)

    with jax.named_scope("w_sends"):
        for copy in (
            xy_2, gather_z, stats_z, gather_y, gather_y2, stats_y, gather_c, gather_c2, stats_c, z_0, z_1, z_2,
            grad_sums, gather_x,
        ):
            copy.wait_send()


def write_out(dx_ref, wg_ref, dx_hbm, wg_hbm, sem):
    copies = [pltpu.make_async_copy(dx_ref, dx_hbm, sem.at[0]), pltpu.make_async_copy(wg_ref, wg_hbm, sem.at[1])]
    for copy in copies:
        copy.start()
    for copy in copies:
        copy.wait()


def on_device(raw_weight, inputs, cotangent):
    rows, taps, chan = raw_weight.shape
    ex, ey, ez = inputs.shape[:3]
    dma = pltpu.SemaphoreType.DMA

    scratch = [
        pltpu.VMEM((taps, rows, chan), F32),
        pltpu.VMEM(inputs.shape, BF16),
        pltpu.VMEM((3, ex + 2, ey + 2, ez, chan), BF16),
        pltpu.VMEM((2, ey + 2, ez, chan), BF16),
        pltpu.VMEM((2, ex + 2, ez, chan), BF16),
        pltpu.VMEM((2, ex + 4, ey, chan), BF16),
        pltpu.VMEM((2, ex + 4, ey, chan), BF16),
        pltpu.VMEM((2, ex, ey, chan), BF16),
        pltpu.VMEM((2, ex, ey, chan), BF16),
        pltpu.VMEM((3, chan, ex * ey * ez), BF16),
        pltpu.VMEM((2, 3, chan, ex * ez), BF16),
        pltpu.VMEM((2, chan, ex * ey), BF16),
        pltpu.VMEM((2, ex + 2, 24, chan), F32),
        pltpu.VMEM((2, 3, ex + 2, ey, chan), BF16),
        pltpu.VMEM((NCORE, taps, chan // NCORE, chan), F32),
        pltpu.VMEM((taps, chan // NCORE, chan), F32),
        pltpu.VMEM((NYC, taps + 1, 16, chan), BF16),
        pltpu.VMEM((NXC * NYC - 1, SLOTS, 16, chan), BF16),
        pltpu.VMEM((NZR, SLOTS, 16, chan), BF16),
        pltpu.VMEM((NXC, SLOTS, rows, chan), F32),
        pltpu.VMEM((NZL, taps, rows, chan), BF16),
        pltpu.VMEM((taps + 1, 8, 16, chan), BF16),
        pltpu.VMEM((chan, taps * chan), BF16),
        pltpu.VMEM(inputs.shape, F32),
        pltpu.VMEM((8, NZL, 2, chan), F32),
        pltpu.VMEM((32, 4, chan), F32),
        dma((3,)), dma((26,)), dma((12,)), dma((19,)), pltpu.SemaphoreType.REGULAR,
    ]
    vmem = pl.BlockSpec(memory_space=pltpu.VMEM)
    anywhere = pl.BlockSpec(memory_space=pl.ANY)
    shapes = (
        jax.ShapeDtypeStruct(cotangent.shape, BF16),
        jax.ShapeDtypeStruct((taps, rows, chan), F32),
    )
    results = pl.pallas_call(
        kernel,
        out_shape=tuple(pltpu.VMEM(one.shape, one.dtype) for one in shapes),
        in_specs=[anywhere] * 3,
        out_specs=(vmem, vmem),
        scratch_shapes=scratch,
        compiler_params=pltpu.CompilerParams(
            collective_id=0, has_side_effects=True, vmem_limit_bytes=32 * 1024 * 1024
        ),
    )(*(
        pltpu.with_memory_space_constraint(one, pltpu.HBM)
        for one in (jnp.transpose(raw_weight, (1, 0, 2)), inputs, cotangent)
    ))
    input_grad, weight_grad = pl.pallas_call(
        write_out,
        out_shape=shapes,
        in_specs=[vmem, vmem],
        out_specs=(anywhere, anywhere),
        scratch_shapes=[dma((2,))],
    )(*(pltpu.with_memory_space_constraint(one, pltpu.VMEM) for one in results))
    return input_grad, jnp.transpose(weight_grad, (1, 0, 2))


def solution(mesh):
    in_specs = (P(("gx", "gy"), None, None), P("gx", "gy", "gz", None), P("gx", "gy", "gz", None))
    out_specs = (P("gx", "gy", "gz", None), P(("gx", "gy"), None, None))
    return jax.shard_map(
        on_device, mesh=mesh, in_specs=in_specs, out_specs=out_specs, check_vma=False
    )
```

```python
import functools

import jax
import jax.numpy as jnp
from jax import lax
from jax.experimental import pallas as pl
from jax.experimental.pallas import tpu as pltpu
from jax.sharding import PartitionSpec as P

var_eps = 1e-05
norm_eps = 1e-06
clip_norm = 600.0
F32 = jnp.float32
BF16 = jnp.bfloat16
MESH = pl.DeviceIdType.MESH
AXES = ("gx", "gy", "gz")

NCORE, NZL, NYC, NXC, NZH = 2, 4, 4, 4, 2
NZR = NZL * NZH
CHUNKS = ((0, 8, 2, 0), (8, 8, 2, 2), (16, 11, 3, 4))
SLOTS = 7
W_SPLIT = 11


def kernel(raw_hbm, in_hbm, cot_hbm, dx_ref, wg_ref, *scratch):
    (raw_ref, in_ref, shifted, halo_x, halo_y, along_out, along_in, in_out, in_in, in_t, edge_y, rim, rim_view,
     part, recv_c, send_xy, recv_xy, recv_z, full, wy, wz, w_all, w_cat, dx_acc, stats_w, stats_g,
     load_sem, sends, halo_recv, recvs, hello) = scratch
    taps, rows, chan = raw_ref.shape
    ex, ey, ez = in_ref.shape[:3]
    fan_count = float(rows * NCORE * NZL * NYC * taps)
    count = {"gx": NCORE * NZL, "gy": NYC, "gz": NXC * NZH}
    me = {axis: lax.axis_index(axis) for axis in AXES}
    core, zl = lax.rem(me["gx"], NCORE), lax.div(me["gx"], NCORE)
    my = me["gy"]
    mx, zh = lax.rem(me["gz"], NXC), lax.div(me["gz"], NXC)
    mz = zh * NZL + zl

    def spot(c=None, x=None, y=None, z=None):
        c = core if c is None else c
        x = mx if x is None else x
        y = my if y is None else y
        z = mz if z is None else z
        return {"gx": lax.rem(z, NZL) * NCORE + c, "gy": y, "gz": lax.div(z, NZL) * NXC + x}

    partner = spot(c=1 - core)
    x_line = [lax.rem(mx + k, NXC) for k in range(1, NXC)]
    y_line = [lax.rem(my + k, NYC) for k in range(1, NYC)]

    def xy_peer(k):
        flat = lax.rem(my * NXC + mx + k, NXC * NYC)
        return lax.rem(flat, NXC), lax.div(flat, NXC)

    flat_g = (my * NXC + mx) * NCORE + core

    def stat_peer(k):
        flat = lax.rem(flat_g + k, 32)
        where = lax.div(flat, NCORE)
        return spot(c=lax.rem(flat, NCORE), x=lax.rem(where, NXC), y=lax.div(where, NXC))

    def z_peer(k):
        return spot(z=lax.rem(mz + k, NZR))

    def remote(src, dst, send_sem, recv_sem, where):
        return pltpu.make_async_remote_copy(
            src_ref=src, dst_ref=dst, send_sem=send_sem, recv_sem=recv_sem,
            device_id=where, device_id_type=MESH,
        )

    def group(copies, wholes, send_sem, recv_sem):
        for src, dst, where in copies:
            remote(src, dst, send_sem, recv_sem, where).start()
        return remote(wholes, wholes, send_sem, recv_sem, partner)

    body = pl.ds(1, ey)
    load_cot = pltpu.make_async_copy(cot_hbm, shifted.at[1, pl.ds(1, ex), body], load_sem.at[0])
    load_in = pltpu.make_async_copy(in_hbm, in_ref, load_sem.at[1])
    load_raw = pltpu.make_async_copy(raw_hbm, raw_ref, load_sem.at[2])
    load_cot.start()
    load_in.start()
    load_raw.start()

    low = {axis: me[axis] == 0 for axis in AXES}
    high = {axis: me[axis] == count[axis] - 1 for axis in AXES}
    plane_offs = [(a, b, 0) for a in (1, -1, 0) for b in (0, 1, -1) if (a, b) != (0, 0)]

    def neighbour(off):
        return {axis: lax.rem(me[axis] + count[axis] + o, count[axis]) for axis, o in zip(AXES, off)}

    def exists(off):
        ok = None
        for axis, o in zip(AXES, off):
            if o != 0:
                one = me[axis] < count[axis] - 1 if o > 0 else me[axis] > 0
                ok = one if ok is None else jnp.logical_and(ok, one)
        return ok

    barrier = pltpu.get_barrier_semaphore()
    for off in [(0, 0, 1), (0, 0, -1)] + plane_offs:

        @pl.when(exists(off))
        def _():
            pl.semaphore_signal(barrier, inc=1, device_id=neighbour(off), device_id_type=MESH)

    near_z = [spot(z=lax.rem(mz + k, NZR)) for k in (1, 2, NZR - 2, NZR - 1)]
    lines = [spot(c=c, x=x) for x in x_line for c in range(NCORE)]
    lines += [spot(c=c, y=y) for y in y_line for c in range(NCORE)]
    for where in near_z + lines:
        pl.semaphore_signal(barrier, inc=1, device_id=where, device_id_type=MESH)

    line_end = jnp.logical_or(zl == 0, zl == NZL - 1)

    @pl.when(line_end)
    def _():
        where = spot(z=zh * NZL + NZL - 1 - zl)
        pl.semaphore_signal(barrier, inc=1, device_id=where, device_id_type=MESH)

    def sides(axis):
        return (me[axis] > 0).astype(jnp.int32), (me[axis] < count[axis] - 1).astype(jnp.int32)

    around = (1 + sum(sides("gx"))) * (1 + sum(sides("gy")))
    greeted = around - 1 + sum(sides("gz")) + len(near_z) + len(lines) + line_end.astype(jnp.int32)

    tile = jnp.zeros((16, chan), BF16)
    for end, at_end in enumerate((low, high)):
        shifted[1, (ex + 1) * end] = jnp.zeros((ey + 2, ez, chan), BF16)
        shifted[1, :, (ey + 1) * end] = jnp.zeros((ex + 2, ez, chan), BF16)
        for side in range(2):
            halo_y[side, (ex + 1) * end] = tile

        @pl.when(at_end["gx"])
        def _():
            halo_x[end] = jnp.zeros((ey + 2, ez, chan), BF16)

        @pl.when(at_end["gy"])
        def _():
            for side in range(2):
                halo_x[side, (ey + 1) * end] = tile
            halo_y[end, 1:ex + 1] = jnp.zeros((ex, ez, chan), BF16)

        @pl.when(at_end["gz"])
        def _():
            in_in[end] = jnp.zeros((chan, ex * ey), BF16)
            along_in[end] = jnp.zeros((ex + 4, ey, chan), BF16)

    w_all[taps] = jnp.zeros((8, 16, chan), BF16)
    for y in range(NYC):
        send_xy[y, taps] = tile
    with jax.named_scope("w_cot"):
        load_cot.wait()

    load_in.wait()
    order = [t for c in (1, 2, 0) for t in range(c, taps, 3)]

    def per_output(value):
        return jnp.sum(jnp.sum(value, axis=0), axis=0, keepdims=True)

    row_i = lax.broadcasted_iota(jnp.int32, (chan, chan), 0)
    col_i = lax.broadcasted_iota(jnp.int32, (chan, chan), 1)

    def natural(i):
        return (i // 4 % 4) * 32 + (i // 64) * 16 + (i // 16 % 4) * 4 + i % 4

    to_mine = jnp.where(col_i == natural(row_i), 1.0, 0.0).astype(BF16)
    to_natural = jnp.where(row_i == natural(col_i), 1.0, 0.0).astype(BF16)

    def transposed(block):
        return lax.dot_general(
            to_mine, block, (((1,), (1,)), ((), ())), preferred_element_type=F32
        ).astype(BF16)

    for f, z in enumerate((0, ez - 1)):
        face = [in_ref[x].astype(F32)[:, z, :] for x in range(ex)]
        in_out[f] = transposed(jnp.concatenate(face, axis=0).astype(BF16))
    with jax.named_scope("w_barrier"):
        pl.semaphore_wait(barrier, greeted)

    def plane_copy(n, off):
        a, b, _ = off
        near = {1: (ex, ey), -1: (1, 1)}
        side = {1: 0, -1: 1}
        if b == 0:
            src, dst = shifted.at[1, near[a][0], body], halo_x.at[side[a], body]
        elif a == 0:
            src, dst = shifted.at[1, pl.ds(1, ex), near[b][1]], halo_y.at[side[b], pl.ds(1, ex)]
        else:
            src, dst = shifted.at[1, near[a][0], near[b][1]], halo_x.at[side[a], 0 if b > 0 else ey + 1]
        return remote(src, dst, sends.at[n], halo_recv.at[n], neighbour(off))

    def z_copies(n, source, target):
        pairs = []
        for f, off in ((1, (0, 0, 1)), (0, (0, 0, -1))):
            copy = remote(source.at[f], target.at[1 - f], sends.at[n + f], halo_recv.at[n + f], neighbour(off))
            pairs.append([(off, copy)])
        return pairs

    plane = [(off, plane_copy(n, off)) for n, off in enumerate(plane_offs)]
    in_lo, in_hi = z_copies(8, in_out, in_in)
    along = sum(z_copies(10, along_out, along_in), [])

    def halo_do(halos, act, flip):
        for off, copy in halos:

            @pl.when(exists(tuple(-o for o in off) if flip else off))
            def _():
                act(copy)

    def halo_start(halos):
        halo_do(halos, lambda copy: copy.start(), False)

    def halo_sent(halos):
        halo_do(halos, lambda copy: copy.wait_send(), False)

    def halo_wait(halos):
        halo_do(halos, lambda copy: copy.wait_recv(), True)

    halo_start(in_hi)
    halo_start(in_lo)
    halo_start(plane)
    for where in near_z + [spot(x=x) for x in x_line]:
        pl.semaphore_signal(hello, inc=1, device_id=where, device_id_type=MESH)
    load_raw.wait()
    raw = raw_ref[...]
    raw_sum = per_output(raw)
    slab = core * NYC + my
    stats_w[slab, zl] = jnp.concatenate([raw_sum, per_output(raw * raw)], axis=0)
    local_mean = raw_sum / float(rows * taps)
    for u, t in enumerate(order):
        value = (raw_ref[t] - local_mean).astype(BF16)
        if u < W_SPLIT:
            wy[my, u] = value
        else:
            wz[zl, u - W_SPLIT] = value
    w1_copies = []
    for k in range(1, NZL):
        where = spot(z=zh * NZL + lax.rem(zl + k, NZL))
        w1_copies.append((wz.at[zl], wz.at[zl], where))
    gather_z = group(w1_copies, wz.at[pl.ds(0, NZL - 1)], sends.at[21], recvs.at[9])
    stats_z = group(
        [(stats_w.at[slab, zl], stats_w.at[slab, zl], where) for _, _, where in w1_copies],
        stats_w.at[slab, pl.ds(0, NZL - 1)], sends.at[22], recvs.at[10],
    )
    early_y = group(
        [(wy.at[my], wy.at[my], spot(y=y)) for y in y_line], wy.at[pl.ds(0, NYC - 1)], sends.at[23], recvs.at[11]
    )
    depth = lax.broadcasted_iota(jnp.int32, (ey, ez, chan), 1)
    for kind in range(3):
        ends = [[], []]
        for x in range(ex):
            block = in_ref[x]
            if kind:
                moved = pltpu.roll(block.astype(F32), ez - 1 if kind == 1 else 1, 1)
                block = jnp.where(depth == (ez - 1 if kind == 1 else 0), 0.0, moved).astype(BF16)
            in_t[kind, :, x * ey * ez:(x + 1) * ey * ez] = transposed(block.reshape(ey * ez, chan))
            ends[0].append(block[0])
            ends[1].append(block[ey - 1])
        for side in range(2):
            edge_y[side, kind] = transposed(jnp.concatenate(ends[side], axis=0))

    def view(slot, t, start, planes):
        a, b = t // 9, (t // 3) % 3
        block = shifted[slot, pl.ds(start + 2 - a, planes), 2 - b:2 - b + ey]
        return block.reshape(planes * ey * ez, chan)

    half_rows = chan // NCORE
    kinds = {1: 0, 2: 1, 0: 2}

    def products(first, last, left, right_of):
        u = first
        while u < last:
            both = [u]
            if u + 1 < last and order[u + 1] % 3 == order[u] % 3:
                both.append(u + 1)
            views = [right_of(order[v]) for v in both]
            right = jnp.concatenate(views, axis=1) if len(views) > 1 else views[0]
            product = jnp.dot(left(order[u]), right, preferred_element_type=F32)
            for j, v in enumerate(both):
                for c in range(NCORE):
                    yield c, v, product[c * half_rows:(c + 1) * half_rows, j * chan:(j + 1) * chan]
            u += len(both)

    def filter_main(first, last):
        for c, v, value in products(first, last, lambda t: in_t[kinds[t % 3]], lambda t: view(1, t, 0, ex)):
            part[c, v] = value

    where_is = {t: v for v, t in enumerate(order)}
    tap_c = (1, 2, 0)

    def filter_side(left, rights, taps_of):
        product = jnp.dot(left, jnp.concatenate(rights, axis=1), preferred_element_type=F32)
        for kind in range(3):
            for j in range(3):
                v = where_is[taps_of(j) + tap_c[kind]]
                for c in range(NCORE):
                    low_row = kind * chan + c * half_rows
                    part[c, v] = part[c, v] + product[low_row:low_row + half_rows, j * chan:(j + 1) * chan]

    def filter_plane():
        for side, a, x in ((1, 0, ex - 1), (0, 2, 0)):
            left = in_t[:, :, x * ey * ez:(x + 1) * ey * ez].reshape(3 * chan, ey * ez)
            rights = [halo_x[side, 2 - b:2 - b + ey].reshape(ey * ez, chan) for b in range(3)]
            filter_side(left, rights, lambda b: a * 9 + b * 3)
        for side, b in ((1, 0), (0, 2)):
            left = edge_y[side].reshape(3 * chan, ex * ez)
            rights = [halo_y[side, 2 - a:2 - a + ex].reshape(ex * ez, chan) for a in range(3)]
            filter_side(left, rights, lambda a: a * 9 + b * 3)

    def fill_plane():
        for side in range(2):
            shifted[1, (ex + 1) * side] = halo_x[side]
            shifted[1, 1:ex + 1, (ey + 1) * side] = halo_y[side, 1:ex + 1]

    def make_rim():
        for x in range(ex + 2):
            plane = shifted[1, x].astype(F32)
            for side, z in enumerate((0, ez - 1)):
                rim[side, x, 0:ey + 2] = plane[:, z, :]
        for side in range(2):
            for b in range(3):
                rim_view[side, b] = rim[side, :, 2 - b:2 - b + ey].astype(BF16)
            along_out[side, 0:ex + 2] = rim_view[side, 1]
            for b in range(2):
                ends = jnp.concatenate([rim[side, :, (ey + 1) * b], jnp.zeros((ey - ex - 2, chan), F32)], axis=0)
                along_out[side, ex + 2 + b] = ends.astype(BF16)

    def filter_rim(side, first, last):
        def rim_of(t):
            a, b = t // 9, (t // 3) % 3
            return rim_view[side, b, 2 - a:2 - a + ex].reshape(ex * ey, chan)

        for c, v, value in products(first, last, lambda t: in_in[side], rim_of):
            part[c, v] = part[c, v] + value

    def core_chunk(n):
        first, done, _, _ = CHUNKS[n]
        span = pl.ds(first, done)
        return group(
            [(part.at[1 - core, span], recv_c.at[span], partner)], recv_c.at[span], sends.at[12 + n], recvs.at[n]
        )

    def xy_chunk(n, copy):
        first, done, each, slot = CHUNKS[n]
        with jax.named_scope("w_core%d" % n):
            copy.wait_recv()
        for v in range(first, first + done):
            total = part[core, v] + recv_c[v]
            for y in range(NYC):
                send_xy[y, v] = total[y * 16:(y + 1) * 16].astype(BF16)
        copies = []
        for k in range(1, NXC * NYC):
            px, py = xy_peer(k)
            copies.append((
                send_xy.at[py, pl.ds(first + px * each, each)], recv_xy.at[k - 1, pl.ds(slot, each)],
                spot(x=px, y=py),
            ))
        return group(copies, recv_xy.at[:, pl.ds(slot, each)], sends.at[15 + n], recvs.at[3 + n])

    def z_chunk(n, copy):
        first, done, each, slot = CHUNKS[n]
        with jax.named_scope("w_xy%d" % n):
            copy.wait_recv()
        span = pl.ds(slot, each)
        total = send_xy[my, pl.ds(first + mx * each, each)].astype(F32)
        for k in range(1, NXC * NYC):
            total = total + recv_xy[k - 1, span].astype(F32)
        recv_z[mz, span] = total.astype(BF16)
        return group(
            [(recv_z.at[mz, span], recv_z.at[mz, span], z_peer(k)) for k in range(1, NZR)],
            recv_z.at[pl.ds(0, NZR - 1), span], sends.at[18 + n], recvs.at[6 + n],
        )

    def shift(slot, side, amount, edge):
        depth = lax.broadcasted_iota(jnp.int32, (ey, ez, chan), 1)
        for x in range(ex + 2):
            plane = shifted[1, x, 1:ey + 1].astype(F32)
            outer = along_in[side, x].astype(F32)[:, None, :]
            shifted[slot, x, 1:ey + 1] = jnp.where(depth == edge, outer, pltpu.roll(plane, amount, 1)).astype(BF16)
        depth = lax.broadcasted_iota(jnp.int32, (ex + 2, ez, chan), 1)
        for b in range(2):
            y = (ey + 1) * b
            plane = shifted[1, :, y].astype(F32)
            outer = along_in[side, ex + 2 + b].astype(F32)[0:ex + 2][:, None, :]
            shifted[slot, :, y] = jnp.where(depth == edge, outer, pltpu.roll(plane, amount, 1)).astype(BF16)

    filter_main(0, taps)
    with jax.named_scope("w_halo_xy"):
        halo_wait(plane)
    filter_plane()
    core_0 = core_chunk(0)
    fill_plane()
    make_rim()
    with jax.named_scope("w_halo_hi"):
        halo_wait(in_hi)
    filter_rim(1, 9, 18)
    core_1 = core_chunk(1)
    with jax.named_scope("w_halo_lo"):
        halo_wait(in_lo)
    filter_rim(0, 18, 27)
    core_2 = core_chunk(2)
    with jax.named_scope("w_hello"):
        pl.semaphore_wait(hello, len(near_z) + len(x_line))
    xy_0 = xy_chunk(0, core_0)
    with jax.named_scope("w_gather_z"):
        gather_z.wait_recv()
        stats_z.wait_recv()
        early_y.wait_recv()
    early_slab = core * NZL + zl
    early = pl.ds(0, W_SPLIT)
    for u in range(W_SPLIT):
        w_all[u, early_slab] = wy[:, u].astype(F32).reshape(16, chan).astype(BF16)
    for u in range(W_SPLIT, taps):
        w_all[u, slab] = wz[:, u - W_SPLIT].astype(F32).reshape(16, chan).astype(BF16)
    early_z = group(
        [(w_all.at[early, early_slab], w_all.at[early, early_slab], where) for _, _, where in w1_copies],
        w_all.at[early, pl.ds(0, NZL - 1)], sends.at[26], recvs.at[19],
    )

    def gather_part(first, last, send, recv):
        span = pl.ds(first, last - first)
        return group(
            [(w_all.at[span, slab], w_all.at[span, slab], spot(y=y)) for y in y_line],
            w_all.at[span, pl.ds(0, NYC - 1)], sends.at[send], recvs.at[recv],
        )

    def share_part(first, last, send, recv):
        slabs = w_all.at[pl.ds(first, last - first), pl.ds(core * NYC, NYC)]
        return group([(slabs, slabs, partner)], slabs, sends.at[send], recvs.at[recv])

    stats_y = group(
        [(stats_w.at[slab], stats_w.at[slab], spot(y=y)) for y in y_line],
        stats_w.at[pl.ds(0, NYC - 1)], sends.at[24], recvs.at[12],
    )
    xy_1 = xy_chunk(1, core_1)
    xy_2 = xy_chunk(2, core_2)
    halo_start(along)
    for halos in (plane, in_hi, in_lo):
        halo_sent(halos)
    z_0 = z_chunk(0, xy_0)
    gather_y2 = gather_part(W_SPLIT, taps, 25, 17)
    z_1 = z_chunk(1, xy_1)
    z_2 = z_chunk(2, xy_2)
    with jax.named_scope("w_gather_y"):
        early_z.wait_recv()
        stats_y.wait_recv()
    core_0.wait_send()
    core_1.wait_send()
    gather_c = share_part(0, W_SPLIT, 12, 13)
    mine = stats_w.at[pl.ds(core * NYC, NYC)]
    stats_c = group([(mine, mine, partner)], mine, sends.at[13], recvs.at[14])

    with jax.named_scope("w_halo_along"):
        halo_wait(along)
        halo_sent(along)
    shift(2, 1, ez - 1, ez - 1)
    shift(0, 0, 1, 0)
    with jax.named_scope("w_gather_c"):
        gather_c.wait_recv()
        stats_c.wait_recv()
    sums = stats_w[0, 0]
    for k in range(1, 32):
        sums = sums + stats_w[k // NZL, k % NZL]
    mean_out = sums[0:1] / fan_count
    var_out = sums[1:2] / fan_count - mean_out * mean_out
    inv_std = lax.rsqrt(var_out + var_eps)
    offset = []
    for k in range(32):
        gap = stats_w[k // NZL, k % NZL][0:1] / float(rows * taps) - mean_out
        offset.append(jnp.broadcast_to(gap, (rows, chan)))
    offset = jnp.concatenate(offset, axis=0)

    natural_slabs = [g % NCORE * NZL + g // NCORE for g in range(NCORE * NZL)]
    early_offset = []
    for g in range(NCORE * NZL):
        for y in range(NYC):
            gap = stats_w[g % NCORE * NYC + y, g // NCORE][0:1] / float(rows * taps) - mean_out
            early_offset.append(jnp.broadcast_to(gap, (rows, chan)))
    early_offset = jnp.concatenate(early_offset, axis=0)
    for u in range(W_SPLIT):
        value = jnp.concatenate([w_all[u, g] for g in natural_slabs], axis=0).astype(F32)
        w_cat[:, u * chan:(u + 1) * chan] = ((value + early_offset) * inv_std).astype(BF16)

    def standardize(first, last):
        for u in range(first, last, 2):
            pair = range(u, min(u + 2, last))
            right = []
            for v in pair:
                value = (w_all[v].reshape(chan, chan).astype(F32) + offset) * inv_std
                right.append(value.astype(BF16))
            right = jnp.concatenate(right, axis=1) if len(right) > 1 else right[0]
            w_cat[:, u * chan:(u + len(pair)) * chan] = jnp.dot(
                to_natural, right, preferred_element_type=F32
            ).astype(BF16)

    def dx_steps(first, last, step, finish):
        def dx_step(n, carry):
            start = n * step
            left = jnp.concatenate([view(2 - t % 3, t, start, step) for t in order[first:last]], axis=1)
            product = lax.dot_general(
                left, w_cat[:, first * chan:last * chan], (((1,), (1,)), ((), ())), preferred_element_type=F32
            )
            finish(pl.ds(start, step), product.reshape(step, ey, ez, chan))
            return carry

        lax.fori_loop(0, ex // step, dx_step, 0)

    def keep(span, value):
        dx_acc[span] = value

    def finish(span, value):
        dx_ref[span] = (value + dx_acc[span]).astype(BF16)

    with jax.named_scope("dxa"):
        dx_steps(0, W_SPLIT, 4, keep)
    with jax.named_scope("w_gather_y2"):
        gather_y2.wait_recv()
    core_2.wait_send()
    gather_c2 = share_part(W_SPLIT, taps, 14, 18)

    pivot = stats_w[slab, 0][0:1]
    gap = [jnp.broadcast_to((stats_w[slab, q][0:1] - pivot) / float(rows * taps), (rows, chan)) for q in range(NZL)]
    gap = jnp.concatenate(gap, axis=0)
    def own_rows(u):
        pieces = []
        for q in range(NZL):
            block = w_all[u, core * NZL + q].astype(F32)
            piece = block[0:rows]
            for y in range(1, NYC):
                piece = jnp.where(my == y, block[y * rows:(y + 1) * rows], piece)
            pieces.append(piece)
        return jnp.concatenate(pieces, axis=0)

    near = []
    for first, done, each, _ in CHUNKS:
        for j in range(each):
            u = first + mx * each + j
            if first + done <= W_SPLIT:
                near.append(own_rows(u))
            elif first >= W_SPLIT:
                near.append(w_all[u, slab].astype(F32))
            else:
                near.append(jnp.where(u < W_SPLIT, own_rows(u), w_all[u, slab].astype(F32)))
    near = [value + gap for value in near]
    grad = []
    with jax.named_scope("w_z"):
        for (_, _, each, slot), copy in zip(CHUNKS, (z_0, z_1, z_2)):
            copy.wait_recv()
            for j in range(slot, slot + each):
                total = recv_z[0, j].astype(F32)
                for k in range(1, NZR):
                    total = total + recv_z[k, j].astype(F32)
                grad.append(total)
    total, cross, square = grad[0], grad[0] * near[0], grad[0] * grad[0]
    for j in range(1, SLOTS):
        total, cross, square = total + grad[j], cross + grad[j] * near[j], square + grad[j] * grad[j]
    stats_g[flat_g] = jnp.concatenate(
        [jnp.sum(value, axis=0, keepdims=True) for value in (total, cross, square)] + [jnp.zeros((1, chan), F32)],
        axis=0,
    )
    xy_0.wait_send()
    xy_1.wait_send()
    grad_sums = group(
        [(stats_g.at[flat_g], stats_g.at[flat_g], stat_peer(k)) for k in range(1, 32)],
        stats_g.at[pl.ds(0, 31)], sends.at[15], recvs.at[15],
    )
    for j in range(SLOTS):
        owned = grad[j][0:rows]
        for q in range(1, NZL):
            owned = jnp.where(zl == q, grad[j][q * rows:(q + 1) * rows], owned)
        full[mx, j] = owned
    gather_x = group(
        [(full.at[mx], full.at[mx], spot(x=x)) for x in x_line],
        full.at[pl.ds(0, NXC - 1)], sends.at[16], recvs.at[16],
    )

    with jax.named_scope("w_gather_c2"):
        gather_c2.wait_recv()
    standardize(W_SPLIT, taps)
    with jax.named_scope("dxb"):
        dx_steps(W_SPLIT, taps, 4, finish)

    with jax.named_scope("w_grad_sums"):
        grad_sums.wait_recv()
    with jax.named_scope("w_gather_x"):
        gather_x.wait_recv()
    sum_grad, sum_cross, sum_square = (jnp.zeros((1, chan), F32) for _ in range(3))
    for k in range(32):
        one = stats_g[k]
        about = stats_w[k % NCORE * NYC + k // (NXC * NCORE), 0][0:1] / float(rows * taps) - mean_out
        sum_grad = sum_grad + one[0:1]
        sum_cross = sum_cross + (one[1:2] + about * one[0:1])
        sum_square = sum_square + one[2:3]
    sum_cross = sum_cross * inv_std
    mean_grad = sum_grad / fan_count
    mean_cross = sum_cross / fan_count
    spread = sum_square - 2.0 * mean_grad * sum_grad - 2.0 * mean_cross * sum_cross
    spread = (
        spread
        + fan_count * mean_grad * mean_grad
        + fan_count * mean_cross * mean_cross * var_out / (var_out + var_eps)
    )
    square_sum = jnp.sum(inv_std * inv_std * spread, axis=1, keepdims=True)
    scale = jnp.minimum(1.0, clip_norm * lax.rsqrt(square_sum + norm_eps))
    factor = inv_std * scale
    for first, done, each, slot in CHUNKS:
        for v in range(done):
            t = order[first + v]
            std = (raw_ref[t] - mean_out) * inv_std
            wg_ref[t] = factor * (full[v // each, slot + v % each] - mean_grad - std * mean_cross)

    with jax.named_scope("w_sends"):
        for copy in (
            xy_2, gather_z, stats_z, early_y, early_z, gather_y2, stats_y, gather_c, gather_c2, stats_c, z_0, z_1, z_2,
            grad_sums, gather_x,
        ):
            copy.wait_send()


def write_out(dx_ref, wg_ref, dx_hbm, wg_hbm, sem):
    copies = [pltpu.make_async_copy(dx_ref, dx_hbm, sem.at[0]), pltpu.make_async_copy(wg_ref, wg_hbm, sem.at[1])]
    for copy in copies:
        copy.start()
    for copy in copies:
        copy.wait()


def on_device(raw_weight, inputs, cotangent):
    rows, taps, chan = raw_weight.shape
    ex, ey, ez = inputs.shape[:3]
    dma = pltpu.SemaphoreType.DMA

    scratch = [
        pltpu.VMEM((taps, rows, chan), F32),
        pltpu.VMEM(inputs.shape, BF16),
        pltpu.VMEM((3, ex + 2, ey + 2, ez, chan), BF16),
        pltpu.VMEM((2, ey + 2, ez, chan), BF16),
        pltpu.VMEM((2, ex + 2, ez, chan), BF16),
        pltpu.VMEM((2, ex + 4, ey, chan), BF16),
        pltpu.VMEM((2, ex + 4, ey, chan), BF16),
        pltpu.VMEM((2, chan, ex * ey), BF16),
        pltpu.VMEM((2, chan, ex * ey), BF16),
        pltpu.VMEM((3, chan, ex * ey * ez), BF16),
        pltpu.VMEM((2, 3, chan, ex * ez), BF16),
        pltpu.VMEM((2, ex + 2, 24, chan), F32),
        pltpu.VMEM((2, 3, ex + 2, ey, chan), BF16),
        pltpu.VMEM((NCORE, taps, chan // NCORE, chan), F32),
        pltpu.VMEM((taps, chan // NCORE, chan), F32),
        pltpu.VMEM((NYC, taps + 1, 16, chan), BF16),
        pltpu.VMEM((NXC * NYC - 1, SLOTS, 16, chan), BF16),
        pltpu.VMEM((NZR, SLOTS, 16, chan), BF16),
        pltpu.VMEM((NXC, SLOTS, rows, chan), F32),
        pltpu.VMEM((NYC, W_SPLIT, rows, chan), BF16),
        pltpu.VMEM((NZL, taps - W_SPLIT, rows, chan), BF16),
        pltpu.VMEM((taps + 1, 8, 16, chan), BF16),
        pltpu.VMEM((chan, taps * chan), BF16),
        pltpu.VMEM(inputs.shape, F32),
        pltpu.VMEM((8, NZL, 2, chan), F32),
        pltpu.VMEM((32, 4, chan), F32),
        dma((3,)), dma((27,)), dma((12,)), dma((20,)), pltpu.SemaphoreType.REGULAR,
    ]
    vmem = pl.BlockSpec(memory_space=pltpu.VMEM)
    anywhere = pl.BlockSpec(memory_space=pl.ANY)
    shapes = (
        jax.ShapeDtypeStruct(cotangent.shape, BF16),
        jax.ShapeDtypeStruct((taps, rows, chan), F32),
    )
    results = pl.pallas_call(
        kernel,
        out_shape=tuple(pltpu.VMEM(one.shape, one.dtype) for one in shapes),
        in_specs=[anywhere] * 3,
        out_specs=(vmem, vmem),
        scratch_shapes=scratch,
        compiler_params=pltpu.CompilerParams(
            collective_id=0, has_side_effects=True, vmem_limit_bytes=32 * 1024 * 1024
        ),
    )(*(
        pltpu.with_memory_space_constraint(one, pltpu.HBM)
        for one in (jnp.transpose(raw_weight, (1, 0, 2)), inputs, cotangent)
    ))
    input_grad, weight_grad = pl.pallas_call(
        write_out,
        out_shape=shapes,
        in_specs=[vmem, vmem],
        out_specs=(anywhere, anywhere),
        scratch_shapes=[dma((2,))],
    )(*(pltpu.with_memory_space_constraint(one, pltpu.VMEM) for one in results))
    return input_grad, jnp.transpose(weight_grad, (1, 0, 2))


def solution(mesh):
    in_specs = (P(("gx", "gy"), None, None), P("gx", "gy", "gz", None), P("gx", "gy", "gz", None))
    out_specs = (P("gx", "gy", "gz", None), P(("gx", "gy"), None, None))
    return jax.shard_map(
        on_device, mesh=mesh, in_specs=in_specs, out_specs=out_specs, check_vma=False
    )
```

```python
import functools

import jax
import jax.numpy as jnp
from jax import lax
from jax.experimental import pallas as pl
from jax.experimental.pallas import tpu as pltpu
from jax.sharding import PartitionSpec as P

var_eps = 1e-05
norm_eps = 1e-06
clip_norm = 600.0
F32 = jnp.float32
BF16 = jnp.bfloat16
MESH = pl.DeviceIdType.MESH
AXES = ("gx", "gy", "gz")

NCORE, NZL, NYC, NXC, NZH = 2, 4, 4, 4, 2
NZR = NZL * NZH
CHUNKS = ((0, 8, 2, 0), (8, 8, 2, 2), (16, 11, 3, 4))
SLOTS = 7
W_SPLIT = 11


def kernel(raw_hbm, in_hbm, cot_hbm, dx_ref, wg_ref, *scratch):
    (raw_ref, in_ref, shifted, halo_x, halo_y, along_out, along_in, in_out, in_in, in_t, edge_y, rim, rim_view,
     part, part_out, recv_c, send_xy, recv_xy, recv_z, full, wy, wz, w_all, w_cat, dx_acc, stats_w, stats_g,
     load_sem, sends, halo_recv, recvs, hello) = scratch
    taps, rows, chan = raw_ref.shape
    ex, ey, ez = in_ref.shape[:3]
    fan_count = float(rows * NCORE * NZL * NYC * taps)
    count = {"gx": NCORE * NZL, "gy": NYC, "gz": NXC * NZH}
    me = {axis: lax.axis_index(axis) for axis in AXES}
    core, zl = lax.rem(me["gx"], NCORE), lax.div(me["gx"], NCORE)
    my = me["gy"]
    mx, zh = lax.rem(me["gz"], NXC), lax.div(me["gz"], NXC)
    mz = zh * NZL + zl

    def spot(c=None, x=None, y=None, z=None):
        c = core if c is None else c
        x = mx if x is None else x
        y = my if y is None else y
        z = mz if z is None else z
        return {"gx": lax.rem(z, NZL) * NCORE + c, "gy": y, "gz": lax.div(z, NZL) * NXC + x}

    partner = spot(c=1 - core)
    x_line = [lax.rem(mx + k, NXC) for k in range(1, NXC)]
    y_line = [lax.rem(my + k, NYC) for k in range(1, NYC)]

    def xy_peer(k):
        flat = lax.rem(my * NXC + mx + k, NXC * NYC)
        return lax.rem(flat, NXC), lax.div(flat, NXC)

    flat_g = (my * NXC + mx) * NCORE + core

    def stat_peer(k):
        flat = lax.rem(flat_g + k, 32)
        where = lax.div(flat, NCORE)
        return spot(c=lax.rem(flat, NCORE), x=lax.rem(where, NXC), y=lax.div(where, NXC))

    def z_peer(k):
        return spot(z=lax.rem(mz + k, NZR))

    def remote(src, dst, send_sem, recv_sem, where):
        return pltpu.make_async_remote_copy(
            src_ref=src, dst_ref=dst, send_sem=send_sem, recv_sem=recv_sem,
            device_id=where, device_id_type=MESH,
        )

    def group(copies, wholes, send_sem, recv_sem):
        for src, dst, where in copies:
            remote(src, dst, send_sem, recv_sem, where).start()
        return remote(wholes, wholes, send_sem, recv_sem, partner)

    body = pl.ds(1, ey)
    load_cot = pltpu.make_async_copy(cot_hbm, shifted.at[1, pl.ds(1, ex), body], load_sem.at[0])
    load_in = pltpu.make_async_copy(in_hbm, in_ref, load_sem.at[1])
    load_raw = pltpu.make_async_copy(raw_hbm, raw_ref, load_sem.at[2])
    load_cot.start()
    load_in.start()
    load_raw.start()

    low = {axis: me[axis] == 0 for axis in AXES}
    high = {axis: me[axis] == count[axis] - 1 for axis in AXES}
    plane_offs = [(a, b, 0) for a in (1, -1, 0) for b in (0, 1, -1) if (a, b) != (0, 0)]

    def neighbour(off):
        return {axis: lax.rem(me[axis] + count[axis] + o, count[axis]) for axis, o in zip(AXES, off)}

    def exists(off):
        ok = None
        for axis, o in zip(AXES, off):
            if o != 0:
                one = me[axis] < count[axis] - 1 if o > 0 else me[axis] > 0
                ok = one if ok is None else jnp.logical_and(ok, one)
        return ok

    barrier = pltpu.get_barrier_semaphore()
    for off in [(0, 0, 1), (0, 0, -1)] + plane_offs:

        @pl.when(exists(off))
        def _():
            pl.semaphore_signal(barrier, inc=1, device_id=neighbour(off), device_id_type=MESH)

    near_z = [spot(z=lax.rem(mz + k, NZR)) for k in (1, 2, NZR - 2, NZR - 1)]
    lines = [spot(c=c, x=x) for x in x_line for c in range(NCORE)]
    lines += [spot(c=c, y=y) for y in y_line for c in range(NCORE)]
    for where in near_z + lines:
        pl.semaphore_signal(barrier, inc=1, device_id=where, device_id_type=MESH)

    line_end = jnp.logical_or(zl == 0, zl == NZL - 1)

    @pl.when(line_end)
    def _():
        where = spot(z=zh * NZL + NZL - 1 - zl)
        pl.semaphore_signal(barrier, inc=1, device_id=where, device_id_type=MESH)

    def sides(axis):
        return (me[axis] > 0).astype(jnp.int32), (me[axis] < count[axis] - 1).astype(jnp.int32)

    around = (1 + sum(sides("gx"))) * (1 + sum(sides("gy")))
    greeted = around - 1 + sum(sides("gz")) + len(near_z) + len(lines) + line_end.astype(jnp.int32)

    tile = jnp.zeros((16, chan), BF16)
    for end, at_end in enumerate((low, high)):
        shifted[1, (ex + 1) * end] = jnp.zeros((ey + 2, ez, chan), BF16)
        shifted[1, :, (ey + 1) * end] = jnp.zeros((ex + 2, ez, chan), BF16)
        for side in range(2):
            halo_y[side, (ex + 1) * end] = tile

        @pl.when(at_end["gx"])
        def _():
            halo_x[end] = jnp.zeros((ey + 2, ez, chan), BF16)

        @pl.when(at_end["gy"])
        def _():
            for side in range(2):
                halo_x[side, (ey + 1) * end] = tile
            halo_y[end, 1:ex + 1] = jnp.zeros((ex, ez, chan), BF16)

        @pl.when(at_end["gz"])
        def _():
            in_in[end] = jnp.zeros((chan, ex * ey), BF16)
            along_in[end] = jnp.zeros((ex + 4, ey, chan), BF16)

    w_all[taps] = jnp.zeros((8, 16, chan), BF16)
    for y in range(NYC):
        send_xy[y, taps] = tile
    with jax.named_scope("w_cot"):
        load_cot.wait()

    load_in.wait()
    order = [t for c in (1, 2, 0) for t in range(c, taps, 3)]

    def per_output(value):
        return jnp.sum(jnp.sum(value, axis=0), axis=0, keepdims=True)

    row_i = lax.broadcasted_iota(jnp.int32, (chan, chan), 0)
    col_i = lax.broadcasted_iota(jnp.int32, (chan, chan), 1)

    def natural(i):
        return (i // 4 % 4) * 32 + (i // 64) * 16 + (i // 16 % 4) * 4 + i % 4

    to_mine = jnp.where(col_i == natural(row_i), 1.0, 0.0).astype(BF16)
    to_natural = jnp.where(row_i == natural(col_i), 1.0, 0.0).astype(BF16)

    def transposed(block):
        return lax.dot_general(
            to_mine, block, (((1,), (1,)), ((), ())), preferred_element_type=F32
        ).astype(BF16)

    for f, z in enumerate((0, ez - 1)):
        face = [in_ref[x].astype(F32)[:, z, :] for x in range(ex)]
        in_out[f] = transposed(jnp.concatenate(face, axis=0).astype(BF16))
    with jax.named_scope("w_barrier"):
        pl.semaphore_wait(barrier, greeted)

    def plane_copy(n, off):
        a, b, _ = off
        near = {1: (ex, ey), -1: (1, 1)}
        side = {1: 0, -1: 1}
        if b == 0:
            src, dst = shifted.at[1, near[a][0], body], halo_x.at[side[a], body]
        elif a == 0:
            src, dst = shifted.at[1, pl.ds(1, ex), near[b][1]], halo_y.at[side[b], pl.ds(1, ex)]
        else:
            src, dst = shifted.at[1, near[a][0], near[b][1]], halo_x.at[side[a], 0 if b > 0 else ey + 1]
        return remote(src, dst, sends.at[n], halo_recv.at[n], neighbour(off))

    def z_copies(n, source, target):
        pairs = []
        for f, off in ((1, (0, 0, 1)), (0, (0, 0, -1))):
            copy = remote(source.at[f], target.at[1 - f], sends.at[n + f], halo_recv.at[n + f], neighbour(off))
            pairs.append([(off, copy)])
        return pairs

    plane = [(off, plane_copy(n, off)) for n, off in enumerate(plane_offs)]
    in_lo, in_hi = z_copies(8, in_out, in_in)
    along = sum(z_copies(10, along_out, along_in), [])

    def halo_do(halos, act, flip):
        for off, copy in halos:

            @pl.when(exists(tuple(-o for o in off) if flip else off))
            def _():
                act(copy)

    def halo_start(halos):
        halo_do(halos, lambda copy: copy.start(), False)

    def halo_sent(halos):
        halo_do(halos, lambda copy: copy.wait_send(), False)

    def halo_wait(halos):
        halo_do(halos, lambda copy: copy.wait_recv(), True)

    halo_start(in_hi)
    halo_start(in_lo)
    halo_start(plane)
    for where in near_z + [spot(x=x) for x in x_line]:
        pl.semaphore_signal(hello, inc=1, device_id=where, device_id_type=MESH)
    load_raw.wait()
    raw = raw_ref[...]
    raw_sum = per_output(raw)
    slab = core * NYC + my
    stats_w[slab, zl] = jnp.concatenate([raw_sum, per_output(raw * raw)], axis=0)
    local_mean = raw_sum / float(rows * taps)
    for u, t in enumerate(order):
        value = (raw_ref[t] - local_mean).astype(BF16)
        if u < W_SPLIT:
            wy[my, u] = value
        else:
            wz[zl, u - W_SPLIT] = value
    w1_copies = []
    for k in range(1, NZL):
        where = spot(z=zh * NZL + lax.rem(zl + k, NZL))
        w1_copies.append((wz.at[zl], wz.at[zl], where))
    gather_z = group(w1_copies, wz.at[pl.ds(0, NZL - 1)], sends.at[21], recvs.at[9])
    stats_z = group(
        [(stats_w.at[slab, zl], stats_w.at[slab, zl], where) for _, _, where in w1_copies],
        stats_w.at[slab, pl.ds(0, NZL - 1)], sends.at[22], recvs.at[10],
    )
    early_y = group(
        [(wy.at[my], wy.at[my], spot(y=y)) for y in y_line], wy.at[pl.ds(0, NYC - 1)], sends.at[23], recvs.at[11]
    )
    depth = lax.broadcasted_iota(jnp.int32, (ey, ez, chan), 1)
    for kind in range(3):
        ends = [[], []]
        for x in range(ex):
            block = in_ref[x]
            if kind:
                moved = pltpu.roll(block.astype(F32), ez - 1 if kind == 1 else 1, 1)
                block = jnp.where(depth == (ez - 1 if kind == 1 else 0), 0.0, moved).astype(BF16)
            in_t[kind, :, x * ey * ez:(x + 1) * ey * ez] = transposed(block.reshape(ey * ez, chan))
            ends[0].append(block[0])
            ends[1].append(block[ey - 1])
        for side in range(2):
            edge_y[side, kind] = transposed(jnp.concatenate(ends[side], axis=0))

    def view(slot, t, start, planes):
        a, b = t // 9, (t // 3) % 3
        block = shifted[slot, pl.ds(start + 2 - a, planes), 2 - b:2 - b + ey]
        return block.reshape(planes * ey * ez, chan)

    half_rows = chan // NCORE
    kinds = {1: 0, 2: 1, 0: 2}

    def products(first, last, left, right_of):
        u = first
        while u < last:
            both = [u]
            if u + 1 < last and order[u + 1] % 3 == order[u] % 3:
                both.append(u + 1)
            views = [right_of(order[v]) for v in both]
            right = jnp.concatenate(views, axis=1) if len(views) > 1 else views[0]
            product = jnp.dot(left(order[u]), right, preferred_element_type=F32)
            for j, v in enumerate(both):
                for c in range(NCORE):
                    yield c, v, product[c * half_rows:(c + 1) * half_rows, j * chan:(j + 1) * chan]
            u += len(both)

    def filter_main(first, last):
        for c, v, value in products(first, last, lambda t: in_t[kinds[t % 3]], lambda t: view(1, t, 0, ex)):
            part[c, v] = value

    where_is = {t: v for v, t in enumerate(order)}
    tap_c = (1, 2, 0)

    def filter_side(left, rights, taps_of):
        product = jnp.dot(left, jnp.concatenate(rights, axis=1), preferred_element_type=F32)
        for kind in range(3):
            for j in range(3):
                v = where_is[taps_of(j) + tap_c[kind]]
                for c in range(NCORE):
                    low_row = kind * chan + c * half_rows
                    part[c, v] = part[c, v] + product[low_row:low_row + half_rows, j * chan:(j + 1) * chan]

    def filter_plane():
        for side, a, x in ((1, 0, ex - 1), (0, 2, 0)):
            left = in_t[:, :, x * ey * ez:(x + 1) * ey * ez].reshape(3 * chan, ey * ez)
            rights = [halo_x[side, 2 - b:2 - b + ey].reshape(ey * ez, chan) for b in range(3)]
            filter_side(left, rights, lambda b: a * 9 + b * 3)
        for side, b in ((1, 0), (0, 2)):
            left = edge_y[side].reshape(3 * chan, ex * ez)
            rights = [halo_y[side, 2 - a:2 - a + ex].reshape(ex * ez, chan) for a in range(3)]
            filter_side(left, rights, lambda a: a * 9 + b * 3)

    def fill_plane():
        for side in range(2):
            shifted[1, (ex + 1) * side] = halo_x[side]
            shifted[1, 1:ex + 1, (ey + 1) * side] = halo_y[side, 1:ex + 1]

    def make_rim():
        for x in range(ex + 2):
            plane = shifted[1, x].astype(F32)
            for side, z in enumerate((0, ez - 1)):
                rim[side, x, 0:ey + 2] = plane[:, z, :]
        for side in range(2):
            for b in range(3):
                rim_view[side, b] = rim[side, :, 2 - b:2 - b + ey].astype(BF16)
            along_out[side, 0:ex + 2] = rim_view[side, 1]
            for b in range(2):
                ends = jnp.concatenate([rim[side, :, (ey + 1) * b], jnp.zeros((ey - ex - 2, chan), F32)], axis=0)
                along_out[side, ex + 2 + b] = ends.astype(BF16)

    def filter_rim(side, first, last):
        def rim_of(t):
            a, b = t // 9, (t // 3) % 3
            return rim_view[side, b, 2 - a:2 - a + ex].reshape(ex * ey, chan)

        for c, v, value in products(first, last, lambda t: in_in[side], rim_of):
            part[c, v] = part[c, v] + value

    def core_chunk(n):
        first, done, _, _ = CHUNKS[n]
        span = pl.ds(first, done)
        part_out[span] = part[1 - core, span].astype(BF16)
        return group(
            [(part_out.at[span], recv_c.at[span], partner)], recv_c.at[span], sends.at[12 + n], recvs.at[n]
        )

    def xy_chunk(n, copy):
        first, done, each, slot = CHUNKS[n]
        with jax.named_scope("w_core%d" % n):
            copy.wait_recv()
        for v in range(first, first + done):
            total = part[core, v] + recv_c[v].astype(F32)
            for y in range(NYC):
                send_xy[y, v] = total[y * 16:(y + 1) * 16].astype(BF16)
        copies = []
        for k in range(1, NXC * NYC):
            px, py = xy_peer(k)
            copies.append((
                send_xy.at[py, pl.ds(first + px * each, each)], recv_xy.at[k - 1, pl.ds(slot, each)],
                spot(x=px, y=py),
            ))
        return group(copies, recv_xy.at[:, pl.ds(slot, each)], sends.at[15 + n], recvs.at[3 + n])

    def z_chunk(n, copy):
        first, done, each, slot = CHUNKS[n]
        with jax.named_scope("w_xy%d" % n):
            copy.wait_recv()
        span = pl.ds(slot, each)
        total = send_xy[my, pl.ds(first + mx * each, each)].astype(F32)
        for k in range(1, NXC * NYC):
            total = total + recv_xy[k - 1, span].astype(F32)
        recv_z[mz, span] = total.astype(BF16)
        return group(
            [(recv_z.at[mz, span], recv_z.at[mz, span], z_peer(k)) for k in range(1, NZR)],
            recv_z.at[pl.ds(0, NZR - 1), span], sends.at[18 + n], recvs.at[6 + n],
        )

    def shift(slot, side, amount, edge):
        depth = lax.broadcasted_iota(jnp.int32, (ey, ez, chan), 1)
        for x in range(ex + 2):
            plane = shifted[1, x, 1:ey + 1].astype(F32)
            outer = along_in[side, x].astype(F32)[:, None, :]
            shifted[slot, x, 1:ey + 1] = jnp.where(depth == edge, outer, pltpu.roll(plane, amount, 1)).astype(BF16)
        depth = lax.broadcasted_iota(jnp.int32, (ex + 2, ez, chan), 1)
        for b in range(2):
            y = (ey + 1) * b
            plane = shifted[1, :, y].astype(F32)
            outer = along_in[side, ex + 2 + b].astype(F32)[0:ex + 2][:, None, :]
            shifted[slot, :, y] = jnp.where(depth == edge, outer, pltpu.roll(plane, amount, 1)).astype(BF16)

    filter_main(0, taps)
    with jax.named_scope("w_halo_xy"):
        halo_wait(plane)
    filter_plane()
    core_0 = core_chunk(0)
    fill_plane()
    make_rim()
    with jax.named_scope("w_halo_hi"):
        halo_wait(in_hi)
    filter_rim(1, 9, 18)
    core_1 = core_chunk(1)
    with jax.named_scope("w_halo_lo"):
        halo_wait(in_lo)
    filter_rim(0, 18, 27)
    core_2 = core_chunk(2)
    with jax.named_scope("w_hello"):
        pl.semaphore_wait(hello, len(near_z) + len(x_line))
    xy_0 = xy_chunk(0, core_0)
    with jax.named_scope("w_gather_z"):
        gather_z.wait_recv()
        stats_z.wait_recv()
        early_y.wait_recv()
    early_slab = core * NZL + zl
    early = pl.ds(0, W_SPLIT)
    for u in range(W_SPLIT):
        w_all[u, early_slab] = wy[:, u].astype(F32).reshape(16, chan).astype(BF16)
    for u in range(W_SPLIT, taps):
        w_all[u, slab] = wz[:, u - W_SPLIT].astype(F32).reshape(16, chan).astype(BF16)
    early_z = group(
        [(w_all.at[early, early_slab], w_all.at[early, early_slab], where) for _, _, where in w1_copies],
        w_all.at[early, pl.ds(0, NZL - 1)], sends.at[26], recvs.at[19],
    )

    def gather_part(first, last, send, recv):
        span = pl.ds(first, last - first)
        return group(
            [(w_all.at[span, slab], w_all.at[span, slab], spot(y=y)) for y in y_line],
            w_all.at[span, pl.ds(0, NYC - 1)], sends.at[send], recvs.at[recv],
        )

    def share_part(first, last, send, recv):
        slabs = w_all.at[pl.ds(first, last - first), pl.ds(core * NYC, NYC)]
        return group([(slabs, slabs, partner)], slabs, sends.at[send], recvs.at[recv])

    stats_y = group(
        [(stats_w.at[slab], stats_w.at[slab], spot(y=y)) for y in y_line],
        stats_w.at[pl.ds(0, NYC - 1)], sends.at[24], recvs.at[12],
    )
    xy_1 = xy_chunk(1, core_1)
    xy_2 = xy_chunk(2, core_2)
    halo_start(along)
    for halos in (plane, in_hi, in_lo):
        halo_sent(halos)
    z_0 = z_chunk(0, xy_0)
    gather_y2 = gather_part(W_SPLIT, taps, 25, 17)
    z_1 = z_chunk(1, xy_1)
    z_2 = z_chunk(2, xy_2)
    with jax.named_scope("w_gather_y"):
        early_z.wait_recv()
        stats_y.wait_recv()
    core_0.wait_send()
    core_1.wait_send()
    gather_c = share_part(0, W_SPLIT, 12, 13)
    mine = stats_w.at[pl.ds(core * NYC, NYC)]
    stats_c = group([(mine, mine, partner)], mine, sends.at[13], recvs.at[14])

    with jax.named_scope("w_halo_along"):
        halo_wait(along)
        halo_sent(along)
    shift(2, 1, ez - 1, ez - 1)
    shift(0, 0, 1, 0)
    with jax.named_scope("w_gather_c"):
        gather_c.wait_recv()
        stats_c.wait_recv()
    sums = stats_w[0, 0]
    for k in range(1, 32):
        sums = sums + stats_w[k // NZL, k % NZL]
    mean_out = sums[0:1] / fan_count
    var_out = sums[1:2] / fan_count - mean_out * mean_out
    inv_std = lax.rsqrt(var_out + var_eps)
    offset = []
    for k in range(32):
        gap = stats_w[k // NZL, k % NZL][0:1] / float(rows * taps) - mean_out
        offset.append(jnp.broadcast_to(gap, (rows, chan)))
    offset = jnp.concatenate(offset, axis=0)

    natural_slabs = [g % NCORE * NZL + g // NCORE for g in range(NCORE * NZL)]
    early_offset = []
    for g in range(NCORE * NZL):
        for y in range(NYC):
            gap = stats_w[g % NCORE * NYC + y, g // NCORE][0:1] / float(rows * taps) - mean_out
            early_offset.append(jnp.broadcast_to(gap, (rows, chan)))
    early_offset = jnp.concatenate(early_offset, axis=0)
    for u in range(W_SPLIT):
        value = jnp.concatenate([w_all[u, g] for g in natural_slabs], axis=0).astype(F32)
        w_cat[:, u * chan:(u + 1) * chan] = ((value + early_offset) * inv_std).astype(BF16)

    def standardize(first, last):
        for u in range(first, last, 2):
            pair = range(u, min(u + 2, last))
            right = []
            for v in pair:
                value = (w_all[v].reshape(chan, chan).astype(F32) + offset) * inv_std
                right.append(value.astype(BF16))
            right = jnp.concatenate(right, axis=1) if len(right) > 1 else right[0]
            w_cat[:, u * chan:(u + len(pair)) * chan] = jnp.dot(
                to_natural, right, preferred_element_type=F32
            ).astype(BF16)

    def dx_steps(first, last, step, finish):
        def dx_step(n, carry):
            start = n * step
            left = jnp.concatenate([view(2 - t % 3, t, start, step) for t in order[first:last]], axis=1)
            product = lax.dot_general(
                left, w_cat[:, first * chan:last * chan], (((1,), (1,)), ((), ())), preferred_element_type=F32
            )
            finish(pl.ds(start, step), product.reshape(step, ey, ez, chan))
            return carry

        lax.fori_loop(0, ex // step, dx_step, 0)

    def keep(span, value):
        dx_acc[span] = value

    def finish(span, value):
        dx_ref[span] = (value + dx_acc[span]).astype(BF16)

    with jax.named_scope("dxa"):
        dx_steps(0, W_SPLIT, 4, keep)
    with jax.named_scope("w_gather_y2"):
        gather_y2.wait_recv()
    core_2.wait_send()
    gather_c2 = share_part(W_SPLIT, taps, 14, 18)

    pivot = stats_w[slab, 0][0:1]
    gap = [jnp.broadcast_to((stats_w[slab, q][0:1] - pivot) / float(rows * taps), (rows, chan)) for q in range(NZL)]
    gap = jnp.concatenate(gap, axis=0)
    def own_rows(u):
        pieces = []
        for q in range(NZL):
            block = w_all[u, core * NZL + q].astype(F32)
            piece = block[0:rows]
            for y in range(1, NYC):
                piece = jnp.where(my == y, block[y * rows:(y + 1) * rows], piece)
            pieces.append(piece)
        return jnp.concatenate(pieces, axis=0)

    near = []
    for first, done, each, _ in CHUNKS:
        for j in range(each):
            u = first + mx * each + j
            if first + done <= W_SPLIT:
                near.append(own_rows(u))
            elif first >= W_SPLIT:
                near.append(w_all[u, slab].astype(F32))
            else:
                near.append(jnp.where(u < W_SPLIT, own_rows(u), w_all[u, slab].astype(F32)))
    near = [value + gap for value in near]
    grad = []
    with jax.named_scope("w_z"):
        for (_, _, each, slot), copy in zip(CHUNKS, (z_0, z_1, z_2)):
            copy.wait_recv()
            for j in range(slot, slot + each):
                total = recv_z[0, j].astype(F32)
                for k in range(1, NZR):
                    total = total + recv_z[k, j].astype(F32)
                grad.append(total)
    total, cross, square = grad[0], grad[0] * near[0], grad[0] * grad[0]
    for j in range(1, SLOTS):
        total, cross, square = total + grad[j], cross + grad[j] * near[j], square + grad[j] * grad[j]
    stats_g[flat_g] = jnp.concatenate(
        [jnp.sum(value, axis=0, keepdims=True) for value in (total, cross, square)] + [jnp.zeros((1, chan), F32)],
        axis=0,
    )
    xy_0.wait_send()
    xy_1.wait_send()
    grad_sums = group(
        [(stats_g.at[flat_g], stats_g.at[flat_g], stat_peer(k)) for k in range(1, 32)],
        stats_g.at[pl.ds(0, 31)], sends.at[15], recvs.at[15],
    )
    for j in range(SLOTS):
        owned = grad[j][0:rows]
        for q in range(1, NZL):
            owned = jnp.where(zl == q, grad[j][q * rows:(q + 1) * rows], owned)
        full[mx, j] = owned
    gather_x = group(
        [(full.at[mx], full.at[mx], spot(x=x)) for x in x_line],
        full.at[pl.ds(0, NXC - 1)], sends.at[16], recvs.at[16],
    )

    with jax.named_scope("w_gather_c2"):
        gather_c2.wait_recv()
    standardize(W_SPLIT, taps)
    with jax.named_scope("dxb"):
        dx_steps(W_SPLIT, taps, 4, finish)

    with jax.named_scope("w_grad_sums"):
        grad_sums.wait_recv()
    with jax.named_scope("w_gather_x"):
        gather_x.wait_recv()
    sum_grad, sum_cross, sum_square = (jnp.zeros((1, chan), F32) for _ in range(3))
    for k in range(32):
        one = stats_g[k]
        about = stats_w[k % NCORE * NYC + k // (NXC * NCORE), 0][0:1] / float(rows * taps) - mean_out
        sum_grad = sum_grad + one[0:1]
        sum_cross = sum_cross + (one[1:2] + about * one[0:1])
        sum_square = sum_square + one[2:3]
    sum_cross = sum_cross * inv_std
    mean_grad = sum_grad / fan_count
    mean_cross = sum_cross / fan_count
    spread = sum_square - 2.0 * mean_grad * sum_grad - 2.0 * mean_cross * sum_cross
    spread = (
        spread
        + fan_count * mean_grad * mean_grad
        + fan_count * mean_cross * mean_cross * var_out / (var_out + var_eps)
    )
    square_sum = jnp.sum(inv_std * inv_std * spread, axis=1, keepdims=True)
    scale = jnp.minimum(1.0, clip_norm * lax.rsqrt(square_sum + norm_eps))
    factor = inv_std * scale
    for first, done, each, slot in CHUNKS:
        for v in range(done):
            t = order[first + v]
            std = (raw_ref[t] - mean_out) * inv_std
            wg_ref[t] = factor * (full[v // each, slot + v % each] - mean_grad - std * mean_cross)

    with jax.named_scope("w_sends"):
        for copy in (
            xy_2, gather_z, stats_z, early_y, early_z, gather_y2, stats_y, gather_c, gather_c2, stats_c, z_0, z_1, z_2,
            grad_sums, gather_x,
        ):
            copy.wait_send()


def write_out(dx_ref, wg_ref, dx_hbm, wg_hbm, sem):
    copies = [pltpu.make_async_copy(dx_ref, dx_hbm, sem.at[0]), pltpu.make_async_copy(wg_ref, wg_hbm, sem.at[1])]
    for copy in copies:
        copy.start()
    for copy in copies:
        copy.wait()


def on_device(raw_weight, inputs, cotangent):
    rows, taps, chan = raw_weight.shape
    ex, ey, ez = inputs.shape[:3]
    dma = pltpu.SemaphoreType.DMA

    scratch = [
        pltpu.VMEM((taps, rows, chan), F32),
        pltpu.VMEM(inputs.shape, BF16),
        pltpu.VMEM((3, ex + 2, ey + 2, ez, chan), BF16),
        pltpu.VMEM((2, ey + 2, ez, chan), BF16),
        pltpu.VMEM((2, ex + 2, ez, chan), BF16),
        pltpu.VMEM((2, ex + 4, ey, chan), BF16),
        pltpu.VMEM((2, ex + 4, ey, chan), BF16),
        pltpu.VMEM((2, chan, ex * ey), BF16),
        pltpu.VMEM((2, chan, ex * ey), BF16),
        pltpu.VMEM((3, chan, ex * ey * ez), BF16),
        pltpu.VMEM((2, 3, chan, ex * ez), BF16),
        pltpu.VMEM((2, ex + 2, 24, chan), F32),
        pltpu.VMEM((2, 3, ex + 2, ey, chan), BF16),
        pltpu.VMEM((NCORE, taps, chan // NCORE, chan), F32),
        pltpu.VMEM((taps, chan // NCORE, chan), BF16),
        pltpu.VMEM((taps, chan // NCORE, chan), BF16),
        pltpu.VMEM((NYC, taps + 1, 16, chan), BF16),
        pltpu.VMEM((NXC * NYC - 1, SLOTS, 16, chan), BF16),
        pltpu.VMEM((NZR, SLOTS, 16, chan), BF16),
        pltpu.VMEM((NXC, SLOTS, rows, chan), F32),
        pltpu.VMEM((NYC, W_SPLIT, rows, chan), BF16),
        pltpu.VMEM((NZL, taps - W_SPLIT, rows, chan), BF16),
        pltpu.VMEM((taps + 1, 8, 16, chan), BF16),
        pltpu.VMEM((chan, taps * chan), BF16),
        pltpu.VMEM(inputs.shape, F32),
        pltpu.VMEM((8, NZL, 2, chan), F32),
        pltpu.VMEM((32, 4, chan), F32),
        dma((3,)), dma((27,)), dma((12,)), dma((20,)), pltpu.SemaphoreType.REGULAR,
    ]
    vmem = pl.BlockSpec(memory_space=pltpu.VMEM)
    anywhere = pl.BlockSpec(memory_space=pl.ANY)
    shapes = (
        jax.ShapeDtypeStruct(cotangent.shape, BF16),
        jax.ShapeDtypeStruct((taps, rows, chan), F32),
    )
    results = pl.pallas_call(
        kernel,
        out_shape=tuple(pltpu.VMEM(one.shape, one.dtype) for one in shapes),
        in_specs=[anywhere] * 3,
        out_specs=(vmem, vmem),
        scratch_shapes=scratch,
        compiler_params=pltpu.CompilerParams(
            collective_id=0, has_side_effects=True, vmem_limit_bytes=32 * 1024 * 1024
        ),
    )(*(
        pltpu.with_memory_space_constraint(one, pltpu.HBM)
        for one in (jnp.transpose(raw_weight, (1, 0, 2)), inputs, cotangent)
    ))
    input_grad, weight_grad = pl.pallas_call(
        write_out,
        out_shape=shapes,
        in_specs=[vmem, vmem],
        out_specs=(anywhere, anywhere),
        scratch_shapes=[dma((2,))],
    )(*(pltpu.with_memory_space_constraint(one, pltpu.VMEM) for one in results))
    return input_grad, jnp.transpose(weight_grad, (1, 0, 2))


def solution(mesh):
    in_specs = (P(("gx", "gy"), None, None), P("gx", "gy", "gz", None), P("gx", "gy", "gz", None))
    out_specs = (P("gx", "gy", "gz", None), P(("gx", "gy"), None, None))
    return jax.shard_map(
        on_device, mesh=mesh, in_specs=in_specs, out_specs=out_specs, check_vma=False
    )
```
